32 devices in a mesh: pod: 1 (over z), dp: 4 (over y), sp: 8 (over x, core).
Axes of the slice: x: 4, y: 4, z: 1, core: 2. Of those that a mesh axis runs over, the one named last changes fastest.
The devices are a block of a 4x4x8 slice.
Arguments:
- images: bfloat16 [48, 256, 56, 64], P(('pod', 'dp'), 'sp')
- w_a: bfloat16 [2, 3, 3, 64, 64], replicated
- norm_a: float32 [2, 2, 64], replicated
- w_down: bfloat16 [3, 3, 64, 128], replicated
- norm_down: float32 [2, 128], replicated
- w_b: bfloat16 [2, 3, 3, 128, 128], replicated
- norm_b: float32 [2, 2, 128], replicated
Outputs:
- output: bfloat16 [48, 128, 28, 128], P(('pod', 'dp'), 'sp')
All inputs are finite; a program needn't handle non-finite values.
Results may differ from the reference program's by a relative error of at most 0.0039231.
Values are sent between devices in bfloat16 or wider.
A program may use at most 768 MiB of HBM per device.

```python
import jax
import jax.numpy as jnp
from jax import lax

BATCH = 48
HEIGHT = 256
WIDTH = 56
CH_A = 64
CH_B = 128
LAYERS_A = 2
LAYERS_B = 2
EPS_VALUE = 1e-5
CONV_DIMS = ('NHWC', 'HWIO', 'NHWC')


def setup_inputs(seed: int = 0, part: int = 0) -> dict:
    base_key = jax.random.key(seed)
    part_key = jax.random.fold_in(base_key, part)
    noise_key, dir_key, scale_key, offset_key, phase_key = jax.random.split(part_key, 5)
    weight_keys = jax.random.split(base_key, 9)
    row_pos = jnp.arange(HEIGHT, dtype=jnp.float32) * (2.0 / (HEIGHT - 1)) - 1.0
    row_col = row_pos[None, :, None, None]
    noise = jax.random.normal(noise_key, (BATCH, HEIGHT, WIDTH, CH_A), jnp.float32)
    chan_dir = jax.random.normal(dir_key, (BATCH, 1, 1, CH_A), jnp.float32)
    img_scale = jax.random.uniform(scale_key, (BATCH, 1, 1, 1), jnp.float32, 0.5, 1.5)
    img_offset = 0.5 * jax.random.normal(offset_key, (BATCH, 1, 1, CH_A), jnp.float32)
    phase = jax.random.uniform(phase_key, (BATCH, 1, 1, CH_A), jnp.float32, 0.0, 6.2831853)
    wave = 0.5 * jnp.sin(row_col * 7.0 + phase)
    x_val = img_scale * (0.7 * noise + row_col * chan_dir + wave) + img_offset
    w_a = jax.random.normal(weight_keys[0], (LAYERS_A, 3, 3, CH_A, CH_A), jnp.float32) * (9 * CH_A) ** -0.5
    norm_a = jnp.stack([jax.random.uniform(weight_keys[1], (LAYERS_A, CH_A), jnp.float32, 0.6, 1.4), 0.3 * jax.random.normal(weight_keys[2], (LAYERS_A, CH_A), jnp.float32)], axis=1)
    w_down = jax.random.normal(weight_keys[3], (3, 3, CH_A, CH_B), jnp.float32) * (9 * CH_A) ** -0.5
    norm_down = jnp.stack([jax.random.uniform(weight_keys[4], (CH_B,), jnp.float32, 0.6, 1.4), 0.3 * jax.random.normal(weight_keys[5], (CH_B,), jnp.float32)])
    w_b = jax.random.normal(weight_keys[6], (LAYERS_B, 3, 3, CH_B, CH_B), jnp.float32) * (9 * CH_B) ** -0.5
    norm_b = jnp.stack([jax.random.uniform(weight_keys[7], (LAYERS_B, CH_B), jnp.float32, 0.6, 1.4), 0.3 * jax.random.normal(weight_keys[8], (LAYERS_B, CH_B), jnp.float32)], axis=1)
    return {'images': x_val.astype(jnp.bfloat16), 'w_a': w_a.astype(jnp.bfloat16), 'norm_a': norm_a, 'w_down': w_down.astype(jnp.bfloat16), 'norm_down': norm_down, 'w_b': w_b.astype(jnp.bfloat16), 'norm_b': norm_b}


def conv_norm(hidden, weight, norm_pair, stride, pads):
    z_val = lax.conv_general_dilated(hidden.astype(jnp.float32), weight.astype(jnp.float32), (stride, stride), pads, dimension_numbers=CONV_DIMS)
    mean_val = jnp.mean(z_val, axis=(0, 1, 2))
    mean_sq = jnp.mean(z_val * z_val, axis=(0, 1, 2))
    inv_std = lax.rsqrt(mean_sq - mean_val * mean_val + EPS_VALUE)
    scaled = norm_pair[0] * (z_val - mean_val) * inv_std + norm_pair[1]
    return jnp.maximum(scaled, 0.0).astype(jnp.bfloat16)


def reference(images, w_a, norm_a, w_down, norm_down, w_b, norm_b):
    def same_step(hidden, layer_args):
        return conv_norm(hidden, layer_args[0], layer_args[1], 1, ((1, 1), (1, 1))), None
    hidden, unused_a = lax.scan(same_step, images, (w_a, norm_a))
    hidden = conv_norm(hidden, w_down, norm_down, 2, ((0, 1), (0, 1)))
    hidden, unused_b = lax.scan(same_step, hidden, (w_b, norm_b))
    return hidden
```

```python
import functools

import jax
import jax.numpy as jnp
from jax import lax
from jax.experimental import pallas as pl
from jax.experimental.pallas import tpu as pltpu
from jax.sharding import PartitionSpec as P

EPS_VALUE = 1e-5
CONV_DIMS = ('NHWC', 'HWIO', 'NHWC')
MESH_ID = pl.DeviceIdType.MESH


def peer_of(step, data_size, group_size):
    total = data_size * group_size
    me = lax.axis_index('dp') * group_size + lax.axis_index('sp')
    other = lax.rem(me + step, total)
    return {'dp': other // group_size, 'sp': lax.rem(other, group_size)}


def sum_kernel(data_size, group_size, part_ref, out_ref, slots, send_sem, recv_sem):
    total = data_size * group_size
    me = lax.axis_index('dp') * group_size + lax.axis_index('sp')
    barrier = pltpu.get_barrier_semaphore()
    for step in range(1, total):
        pl.semaphore_signal(barrier, inc=1, device_id=peer_of(step, data_size, group_size), device_id_type=MESH_ID)
    slots[me] = part_ref[...]
    pl.semaphore_wait(barrier, total - 1)
    for step in range(1, total):
        pltpu.make_async_remote_copy(src_ref=part_ref, dst_ref=slots.at[me], send_sem=send_sem, recv_sem=recv_sem,
                                     device_id=peer_of(step, data_size, group_size), device_id_type=MESH_ID).start()
    others = slots.at[pl.ds(0, total - 1)]
    pltpu.make_async_copy(others, others, recv_sem).wait()
    out_ref[...] = jnp.sum(slots[...], axis=0)
    pltpu.make_async_copy(others, others, send_sem).wait()


def group_sum(part, data_size, group_size, collective_id):
    total = data_size * group_size
    return pl.pallas_call(
        functools.partial(sum_kernel, data_size, group_size),
        out_shape=jax.ShapeDtypeStruct(part.shape, jnp.float32),
        in_specs=[pl.BlockSpec(memory_space=pltpu.VMEM)],
        out_specs=pl.BlockSpec(memory_space=pltpu.VMEM),
        scratch_shapes=[pltpu.VMEM((total,) + part.shape, jnp.float32), pltpu.SemaphoreType.DMA, pltpu.SemaphoreType.DMA],
        compiler_params=pltpu.CompilerParams(collective_id=collective_id, has_side_effects=True),
        name='group_sum',
    )(part)


def solution(mesh):
    group_size = mesh.shape['sp']
    data_size = mesh.shape['dp']
    to_lower = [(dev_idx, dev_idx + 1) for dev_idx in range(group_size - 1)]
    to_upper = [(dev_idx + 1, dev_idx) for dev_idx in range(group_size - 1)]

    def batch_norm(z_val, norm_pair):
        channels = z_val.shape[-1]
        local_sums = jnp.stack([jnp.sum(z_val, axis=(0, 1, 2)), jnp.sum(z_val * z_val, axis=(0, 1, 2))])
        local_sums = jnp.pad(local_sums, ((0, 0), (0, 128 - channels)))
        group_sums = group_sum(local_sums, data_size, group_size, 0)[:, :channels]
        elem_count = z_val.shape[0] * z_val.shape[1] * z_val.shape[2] * data_size * group_size
        mean_val = group_sums[0] / elem_count
        var_val = group_sums[1] / elem_count - mean_val * mean_val
        scaled = norm_pair[0] * (z_val - mean_val) * lax.rsqrt(var_val + EPS_VALUE) + norm_pair[1]
        return jnp.maximum(scaled, 0.0).astype(jnp.bfloat16)

    def same_layer(hidden, weight, norm_pair):
        top_rows = lax.ppermute(hidden[:, -1:], 'sp', to_lower)
        bottom_rows = lax.ppermute(hidden[:, :1], 'sp', to_upper)
        padded = jnp.concatenate([top_rows, hidden, bottom_rows], axis=1)
        z_val = lax.conv_general_dilated(padded, weight, (1, 1), ((0, 0), (1, 1)), dimension_numbers=CONV_DIMS, preferred_element_type=jnp.float32)
        return batch_norm(z_val, norm_pair)

    def down_layer(hidden, weight, norm_pair):
        bottom_rows = lax.ppermute(hidden[:, :1], 'sp', to_upper)
        padded = jnp.concatenate([hidden, bottom_rows], axis=1)
        z_val = lax.conv_general_dilated(padded, weight, (2, 2), ((0, 0), (0, 1)), dimension_numbers=CONV_DIMS, preferred_element_type=jnp.float32)
        return batch_norm(z_val, norm_pair)

    def local_stack(row_tile, w_a, norm_a, w_down, norm_down, w_b, norm_b):
        hidden = row_tile
        for layer_idx in range(w_a.shape[0]):
            hidden = same_layer(hidden, w_a[layer_idx], norm_a[layer_idx])
        hidden = down_layer(hidden, w_down, norm_down)
        for layer_idx in range(w_b.shape[0]):
            hidden = same_layer(hidden, w_b[layer_idx], norm_b[layer_idx])
        return hidden

    act_spec = P(('pod', 'dp'), 'sp', None, None)
    return jax.shard_map(local_stack, mesh=mesh, in_specs=(act_spec, P(), P(), P(), P(), P(), P()), out_specs=act_spec, check_vma=False)
```

```python
import functools

import jax
import jax.numpy as jnp
from jax import lax
from jax.experimental import pallas as pl
from jax.experimental.pallas import tpu as pltpu
from jax.sharding import PartitionSpec as P

EPS_VALUE = 1e-5
MESH_ID = pl.DeviceIdType.MESH
LANES = 128
HALO = 3
GUARD = 8
F32 = jnp.float32
BF16 = jnp.bfloat16


def stack_kernel(data_size, group_size, images, w_a, norm_a, w_down, norm_down, w_b, norm_b, out,
                 x_in, w_a_in, w_down_in, w_b_in, wide_a, wide_down, wide_b, pixels, masks, taps, z_a, z_down, z_b, z_last,
                 out_rows, parts, slots, in_sems, w_sems, out_sems, image_send, image_recv, z_send, z_recv, sum_send, sum_recv):
    n_img, rows, width, _ = images.shape
    half = width // 2
    block = n_img * half
    pairs = rows // 2
    total = data_size * group_size
    dp_idx = lax.axis_index('dp')
    sp_idx = lax.axis_index('sp')
    me = dp_idx * group_size + sp_idx
    is_top = sp_idx == 0
    is_bottom = sp_idx == group_size - 1

    def peer_of(step):
        other = lax.rem(me + step, total)
        return {'dp': other // group_size, 'sp': lax.rem(other, group_size)}

    barrier = pltpu.get_barrier_semaphore()
    for step in range(1, total):
        pl.semaphore_signal(barrier, inc=1, device_id=peer_of(step), device_id_type=MESH_ID)

    n_chunk = in_sems.shape[0]
    chunk = rows // n_chunk

    def image_copy(idx):
        return pltpu.make_async_copy(images.at[:, pl.ds(idx * chunk, chunk)], x_in.at[:, pl.ds(HALO + idx * chunk, chunk)], in_sems.at[idx])

    for idx in range(n_chunk):
        image_copy(idx).start()
    weight_copies = [pltpu.make_async_copy(w_a, w_a_in, w_sems.at[0]), pltpu.make_async_copy(w_down, w_down_in, w_sems.at[1]),
                     pltpu.make_async_copy(w_b, w_b_in, w_sems.at[2])]
    for copy in weight_copies:
        copy.start()

    pos = lax.rem(lax.broadcasted_iota(jnp.int32, (block, LANES), 0), half)
    masks[0] = (pos != 0).astype(F32)
    masks[1] = (pos != half - 1).astype(F32)
    pixels[0:GUARD] = jnp.zeros((GUARD, LANES), F32)
    pixels[GUARD + n_img * width:] = jnp.zeros((GUARD, LANES), F32)

    def clear_guards(ref, outer):
        def body(idx, carry):
            view = ref.at[idx]
            view[0:GUARD] = jnp.zeros((GUARD, LANES), F32)
            view[GUARD + block:] = jnp.zeros((GUARD, LANES), F32)
            return carry
        lax.fori_loop(0, outer, body, 0)

    clear_guards(z_a, z_a.shape[0])

    def clear_inner(ref):
        def body(idx, carry):
            view = ref.at[idx]
            view[0:GUARD] = jnp.zeros((GUARD, LANES), F32)
            view[GUARD + block:] = jnp.zeros((GUARD, LANES), F32)
            return carry
        lax.fori_loop(1, pairs + 1, body, 0)

    clear_inner(z_down)
    clear_inner(z_b)

    @pl.when(is_top)
    def _():
        x_in[:, 0:HALO] = jnp.zeros((n_img, HALO, width, x_in.shape[3]), BF16)
        z_down[0] = jnp.zeros(z_down.shape[1:], F32)
        z_b[0] = jnp.zeros(z_b.shape[1:], F32)

    @pl.when(is_bottom)
    def _():
        x_in[:, HALO + rows:] = jnp.zeros((n_img, HALO, width, x_in.shape[3]), BF16)
        z_down[pairs + 1] = jnp.zeros(z_down.shape[1:], F32)
        z_b[pairs + 1] = jnp.zeros(z_b.shape[1:], F32)

    pl.semaphore_wait(barrier, total - 1)

    def image_down():
        return pltpu.make_async_remote_copy(src_ref=images.at[:, pl.ds(rows - HALO, HALO)], dst_ref=x_in.at[:, pl.ds(0, HALO)],
                                            send_sem=image_send.at[0], recv_sem=image_recv.at[0],
                                            device_id={'sp': sp_idx + 1}, device_id_type=MESH_ID)

    def image_up():
        return pltpu.make_async_remote_copy(src_ref=images.at[:, pl.ds(0, HALO)], dst_ref=x_in.at[:, pl.ds(HALO + rows, HALO)],
                                            send_sem=image_send.at[1], recv_sem=image_recv.at[1],
                                            device_id={'sp': sp_idx - 1}, device_id_type=MESH_ID)

    @pl.when(jnp.logical_not(is_bottom))
    def _():
        image_down().start()

    @pl.when(jnp.logical_not(is_top))
    def _():
        image_up().start()

    for copy in weight_copies:
        copy.wait()
    ch_a = w_a.shape[3]
    zero_a = jnp.zeros((ch_a, ch_a), BF16)
    zero_b = jnp.zeros((LANES, LANES), BF16)
    zero_d = jnp.zeros((ch_a, LANES), BF16)

    def tap_a(layer, p, q):
        return w_a_in[layer, p, q] if 0 <= p <= 2 and 0 <= q <= 2 else zero_a

    for layer in range(2):
        for q in range(4):
            for t in range(4):
                for dw in range(2):
                    both = jnp.concatenate([tap_a(layer, t, q - dw), tap_a(layer, t - 1, q - dw)], axis=1)
                    wide_a[layer, pl.ds((q * 4 + t) * ch_a, ch_a), pl.ds(dw * LANES, LANES)] = both
    for q in range(3):
        for t in range(6):
            for d in range(2):
                p = t - 1 - 2 * d
                wide_down[pl.ds((q * 6 + t) * ch_a, ch_a), pl.ds(d * LANES, LANES)] = w_down_in[p, q] if 0 <= p <= 2 else zero_d
    for layer in range(2):
        for q in range(3):
            for t in range(4):
                for d in range(2):
                    p = t - d
                    wide_b[layer, pl.ds((q * 4 + t) * LANES, LANES), pl.ds(d * LANES, LANES)] = w_b_in[layer, p, q] if 0 <= p <= 2 else zero_b

    def spread_pair(p, carry):
        upper = x_in[:, 2 * p].astype(F32)
        lower = x_in[:, 2 * p + 1].astype(F32)
        both = jnp.concatenate([upper, lower], axis=2)
        pixels[pl.ds(GUARD, n_img * width)] = both.reshape(n_img * width, LANES)
        taps[0, p] = (pixels[pl.ds(GUARD - 1, block, stride=2)] * masks[0]).astype(BF16)
        taps[1, p] = pixels[pl.ds(GUARD, block, stride=2)].astype(BF16)
        taps[2, p] = pixels[pl.ds(GUARD + 1, block, stride=2)].astype(BF16)
        taps[3, p] = (pixels[pl.ds(GUARD + 2, block, stride=2)] * masks[1]).astype(BF16)
        return carry

    def conv_a(layer, idx):
        left = jnp.concatenate([taps[q, idx + s] for q in range(4) for s in range(2)], axis=1)
        z_val = jnp.dot(left, wide_a[layer], preferred_element_type=F32)
        z_a[idx, pl.ds(GUARD, block)] = z_val[:, :LANES]
        z_a[idx + pairs + 2, pl.ds(GUARD, block)] = z_val[:, LANES:]
        return z_val

    def conv_down(idx):
        left = jnp.concatenate([taps[q, 2 * idx + s] for q in range(1, 4) for s in range(3)], axis=1)
        z_val = jnp.dot(left, wide_down[...], preferred_element_type=F32)
        z_down[2 * idx + 1, pl.ds(GUARD, block)] = z_val[:, :LANES]
        z_down[2 * idx + 2, pl.ds(GUARD, block)] = z_val[:, LANES:]
        return z_val

    def conv_b(layer, idx, dst):
        left = jnp.concatenate([taps[q, 2 * idx + t] for q in range(3) for t in range(4)], axis=1)
        z_val = jnp.dot(left, wide_b[layer], preferred_element_type=F32)
        dst[2 * idx + 1, pl.ds(GUARD, block)] = z_val[:, :LANES]
        dst[2 * idx + 2, pl.ds(GUARD, block)] = z_val[:, LANES:]
        return z_val

    def add_sums(sums, z_val):
        tiles = z_val.reshape(block // 8, 8, 2 * LANES)
        return sums[0] + jnp.sum(tiles, axis=0), sums[1] + jnp.sum(tiles * tiles, axis=0)

    zero_sums = (jnp.zeros((8, 2 * LANES), F32), jnp.zeros((8, 2 * LANES), F32))

    def fold_sums(sums):
        rows_sum = [jnp.sum(val, axis=0, keepdims=True) for val in sums]
        return jnp.concatenate([val[:, :LANES] + val[:, LANES:] for val in rows_sum], axis=0)

    def sum_copy(layer, step):
        return pltpu.make_async_remote_copy(src_ref=parts.at[layer], dst_ref=slots.at[layer, me], send_sem=sum_send.at[layer],
                                            recv_sem=sum_recv.at[layer], device_id=peer_of(step), device_id_type=MESH_ID)

    def group_sum(layer, part):
        parts[layer] = part
        slots[layer, me] = part
        for step in range(1, total):
            sum_copy(layer, step).start()
        others = slots.at[layer, pl.ds(0, total - 1)]
        pltpu.make_async_copy(others, others, sum_recv.at[layer]).wait()
        return jnp.sum(slots[layer], axis=0)

    def finish_sum(layer):
        others = slots.at[layer, pl.ds(0, total - 1)]
        pltpu.make_async_copy(others, others, sum_send.at[layer]).wait()

    def scales(sums, count, gamma, beta):
        mean = sums[0:1] / count
        var = sums[1:2] / count - mean * mean
        return mean, gamma * lax.rsqrt(var + EPS_VALUE), beta

    def scales_a(sums, count, pair):
        both = sums + jnp.concatenate([sums[:, LANES // 2:], sums[:, :LANES // 2]], axis=1)
        twice = jnp.concatenate([pair, pair], axis=1)
        return scales(both, count, twice[0:1], twice[1:2])

    def normed(z_val, scale, keep=None):
        mean, gain, beta = scale
        if keep is not None:
            gain, beta = gain * keep, beta * keep
        return jnp.maximum((z_val - mean) * gain + beta, 0.0)

    keep_top = jnp.where(is_top, 0.0, 1.0).astype(F32)
    keep_bottom = jnp.where(is_bottom, 0.0, 1.0).astype(F32)
    lane = lax.broadcasted_iota(jnp.int32, (1, LANES), 1)
    upper_half = (lane < LANES // 2).astype(F32)
    lower_half = 1.0 - upper_half
    odd = pairs + 2

    for idx in range(n_chunk):
        image_copy(idx).wait()
    lax.fori_loop(2, pairs + 1, spread_pair, 0)
    sums = lax.fori_loop(2, pairs, lambda idx, acc: add_sums(acc, conv_a(0, idx)), zero_sums)

    @pl.when(jnp.logical_not(is_top))
    def _():
        image_down().wait_recv()

    @pl.when(jnp.logical_not(is_bottom))
    def _():
        image_up().wait_recv()

    lax.fori_loop(0, 2, spread_pair, 0)
    lax.fori_loop(pairs + 1, pairs + 3, spread_pair, 0)
    lax.fori_loop(0, 2, lambda idx, acc: (conv_a(0, idx * (pairs + 1)), acc)[1], 0)
    sums = lax.fori_loop(0, 2, lambda idx, acc: add_sums(acc, conv_a(0, 1 + idx * (pairs - 1))), sums)
    count_a = n_img * rows * width * total
    scale = scales_a(group_sum(0, fold_sums(sums)), count_a, norm_a[0])

    def taps_mid(scale, mid):
        def body(idx, carry):
            keep = mid(idx)
            taps[0, idx] = (normed(z_a[idx + odd, pl.ds(GUARD - 1, block)], scale, keep) * masks[0]).astype(BF16)
            taps[1, idx] = normed(z_a[idx, pl.ds(GUARD, block)], scale, keep).astype(BF16)
            taps[2, idx] = normed(z_a[idx + odd, pl.ds(GUARD, block)], scale, keep).astype(BF16)
            taps[3, idx] = (normed(z_a[idx, pl.ds(GUARD + 1, block)], scale, keep) * masks[1]).astype(BF16)
            return carry
        return body

    def keep_pairs(idx):
        return jnp.where(idx == 0, keep_top, jnp.where(idx == pairs + 1, keep_bottom, 1.0))

    lax.fori_loop(0, pairs + 2, taps_mid(scale, keep_pairs), 0)

    def sums_mid(idx, acc):
        z_val = conv_a(1, idx)
        own = jnp.where(idx == 0, lower_half, jnp.where(idx == pairs, upper_half, jnp.ones_like(lower_half)))
        own = jnp.concatenate([own, own], axis=1)
        new = add_sums(zero_sums, z_val)
        return acc[0] + own * new[0], acc[1] + own * new[1]

    sums = lax.fori_loop(0, pairs + 1, sums_mid, zero_sums)
    scale = scales_a(group_sum(1, fold_sums(sums)), count_a, norm_a[1])

    def keep_staggered(idx):
        return jnp.where(idx == pairs, upper_half + lower_half * keep_bottom, jnp.ones_like(lower_half))

    lax.fori_loop(0, pairs + 1, taps_mid(scale, keep_staggered), 0)
    sums = lax.fori_loop(0, pairs // 2, lambda idx, acc: add_sums(acc, conv_down(idx)), zero_sums)

    def edge_copies(ref, slot):
        below = pltpu.make_async_remote_copy(src_ref=ref.at[pairs], dst_ref=ref.at[0], send_sem=z_send.at[slot, 0], recv_sem=z_recv.at[slot, 0],
                                             device_id={'sp': sp_idx + 1}, device_id_type=MESH_ID)
        above = pltpu.make_async_remote_copy(src_ref=ref.at[1], dst_ref=ref.at[pairs + 1], send_sem=z_send.at[slot, 1], recv_sem=z_recv.at[slot, 1],
                                             device_id={'sp': sp_idx - 1}, device_id_type=MESH_ID)
        return below, above

    def send_edges(ref, slot):
        below, above = edge_copies(ref, slot)

        @pl.when(jnp.logical_not(is_bottom))
        def _():
            below.start()

        @pl.when(jnp.logical_not(is_top))
        def _():
            above.start()

    def recv_edges(ref, slot):
        below, above = edge_copies(ref, slot)

        @pl.when(jnp.logical_not(is_top))
        def _():
            below.wait_recv()

        @pl.when(jnp.logical_not(is_bottom))
        def _():
            above.wait_recv()

    def finish_edges(ref, slot):
        below, above = edge_copies(ref, slot)

        @pl.when(jnp.logical_not(is_bottom))
        def _():
            below.wait_send()

        @pl.when(jnp.logical_not(is_top))
        def _():
            above.wait_send()

    count_b = n_img * pairs * half * total
    send_edges(z_down, 0)
    sums_d = group_sum(2, fold_sums(sums))
    scale = scales(sums_d, count_b, norm_down[0:1], norm_down[1:2])
    recv_edges(z_down, 0)

    def taps_low(src, scale):
        def body(idx, carry):
            keep = jnp.where(idx == 0, keep_top, jnp.where(idx == pairs + 1, keep_bottom, 1.0))
            taps[0, idx] = (normed(src[idx, pl.ds(GUARD - 1, block)], scale, keep) * masks[0]).astype(BF16)
            taps[1, idx] = normed(src[idx, pl.ds(GUARD, block)], scale, keep).astype(BF16)
            taps[2, idx] = (normed(src[idx, pl.ds(GUARD + 1, block)], scale, keep) * masks[1]).astype(BF16)
            return carry
        return body

    lax.fori_loop(0, pairs + 2, taps_low(z_down, scale), 0)
    sums = lax.fori_loop(0, pairs // 2, lambda idx, acc: add_sums(acc, conv_b(0, idx, z_b)), zero_sums)
    send_edges(z_b, 1)
    sums_b = group_sum(3, fold_sums(sums))
    scale = scales(sums_b, count_b, norm_b[0, 0:1], norm_b[0, 1:2])
    recv_edges(z_b, 1)
    lax.fori_loop(0, pairs + 2, taps_low(z_b, scale), 0)
    sums = lax.fori_loop(0, pairs // 2, lambda idx, acc: add_sums(acc, conv_b(1, idx, z_last)), zero_sums)
    sums_b = group_sum(4, fold_sums(sums))
    scale = scales(sums_b, count_b, norm_b[1, 0:1], norm_b[1, 1:2])

    n_out = out_sems.shape[0]
    out_chunk = pairs // n_out

    def out_copy(idx):
        return pltpu.make_async_copy(out_rows.at[:, pl.ds(idx * out_chunk, out_chunk)], out.at[:, pl.ds(idx * out_chunk, out_chunk)], out_sems.at[idx])

    def out_body(row, carry):
        for img in range(n_img):
            out_rows[img, row] = normed(z_last[row + 1, pl.ds(GUARD + img * half, half)], scale).astype(BF16)
        return carry

    for idx in range(n_out):
        lax.fori_loop(idx * out_chunk, (idx + 1) * out_chunk, out_body, 0)
        out_copy(idx).start()

    @pl.when(jnp.logical_not(is_bottom))
    def _():
        image_down().wait_send()

    @pl.when(jnp.logical_not(is_top))
    def _():
        image_up().wait_send()

    finish_edges(z_down, 0)
    finish_edges(z_b, 1)
    for layer in range(5):
        finish_sum(layer)
    for idx in range(n_out):
        out_copy(idx).wait()


def solution(mesh):
    group_size = mesh.shape['sp']
    data_size = mesh.shape['dp']
    total = data_size * group_size

    def local_stack(images, w_a, norm_a, w_down, norm_down, w_b, norm_b):
        n_img, rows, width, ch_a = images.shape
        ch_b = w_down.shape[3]
        pairs, half = rows // 2, width // 2
        block = n_img * half
        padded = block + 2 * GUARD
        any_spec = pl.BlockSpec(memory_space=pl.ANY)
        vmem_spec = pl.BlockSpec(memory_space=pltpu.VMEM)
        n_chunk, n_out = 4, 4
        return pl.pallas_call(
            functools.partial(stack_kernel, data_size, group_size),
            out_shape=jax.ShapeDtypeStruct((n_img, pairs, half, ch_b), BF16),
            in_specs=[any_spec, any_spec, vmem_spec, any_spec, vmem_spec, any_spec, vmem_spec],
            out_specs=any_spec,
            scratch_shapes=[
                pltpu.VMEM((n_img, rows + 2 * HALO, width, ch_a), BF16),
                pltpu.VMEM(w_a.shape, BF16),
                pltpu.VMEM(w_down.shape, BF16),
                pltpu.VMEM(w_b.shape, BF16),
                pltpu.VMEM((2, 16 * ch_a, 2 * LANES), BF16),
                pltpu.VMEM((18 * ch_a, 2 * LANES), BF16),
                pltpu.VMEM((2, 12 * ch_b, 2 * LANES), BF16),
                pltpu.VMEM((n_img * width + 2 * GUARD, LANES), F32),
                pltpu.VMEM((2, block, LANES), F32),
                pltpu.VMEM((4, pairs + 3, block, LANES), BF16),
                pltpu.VMEM((2 * (pairs + 2), padded, LANES), F32),
                pltpu.VMEM((pairs + 2, padded, LANES), F32),
                pltpu.VMEM((pairs + 2, padded, LANES), F32),
                pltpu.VMEM((pairs + 2, padded, LANES), F32),
                pltpu.VMEM((n_img, pairs, half, ch_b), BF16),
                pltpu.VMEM((5, 2, LANES), F32),
                pltpu.VMEM((5, total, 2, LANES), F32),
                pltpu.SemaphoreType.DMA((n_chunk,)),
                pltpu.SemaphoreType.DMA((3,)),
                pltpu.SemaphoreType.DMA((n_out,)),
                pltpu.SemaphoreType.DMA((2,)),
                pltpu.SemaphoreType.DMA((2,)),
                pltpu.SemaphoreType.DMA((2, 2)),
                pltpu.SemaphoreType.DMA((2, 2)),
                pltpu.SemaphoreType.DMA((5,)),
                pltpu.SemaphoreType.DMA((5,)),
            ],
            compiler_params=pltpu.CompilerParams(collective_id=0, has_side_effects=True, vmem_limit_bytes=60 * 1024 * 1024),
            name='conv_stack',
        )(images, w_a, norm_a, w_down, norm_down, w_b, norm_b)

    act_spec = P(('pod', 'dp'), 'sp', None, None)
    return jax.shard_map(local_stack, mesh=mesh, in_specs=(act_spec, P(), P(), P(), P(), P(), P()), out_specs=act_spec, check_vma=False)
```

```python
import functools

import jax
import jax.numpy as jnp
from jax import lax
from jax.experimental import pallas as pl
from jax.experimental.pallas import tpu as pltpu
from jax.sharding import PartitionSpec as P

EPS_VALUE = 1e-5
MESH_ID = pl.DeviceIdType.MESH
LANES = 128
HALO = 3
GUARD = 8
F32 = jnp.float32
BF16 = jnp.bfloat16


def stack_kernel(data_size, group_size, images, w_a, norm_a, w_down, norm_down, w_b, norm_b, out,
                 x_in, w_a_in, w_down_in, w_b_in, wide_a, wide_down, wide_b, pixels, masks, taps, z_a, z_mid, z_down, z_b, z_last,
                 out_rows, parts, slots, in_sems, w_sems, out_sems, image_send, image_recv, z_send, z_recv, sum_send, sum_recv):
    n_img, rows, width, _ = images.shape
    half = width // 2
    last_stride = n_img * half + 1
    block = n_img * half
    pairs = rows // 2
    total = data_size * group_size
    dp_idx = lax.axis_index('dp')
    sp_idx = lax.axis_index('sp')
    me = dp_idx * group_size + sp_idx
    is_top = sp_idx == 0
    is_bottom = sp_idx == group_size - 1

    def peer_of(step):
        other = lax.rem(me + step, total)
        return {'dp': other // group_size, 'sp': lax.rem(other, group_size)}

    n_chunk = in_sems.shape[0]
    chunk = rows // n_chunk

    def image_copy(idx):
        return pltpu.make_async_copy(images.at[:, pl.ds(idx * chunk, chunk)], x_in.at[:, pl.ds(HALO + idx * chunk, chunk)], in_sems.at[idx])

    for idx in range(n_chunk):
        image_copy(idx).start()
    weight_copies = [pltpu.make_async_copy(w_a, w_a_in, w_sems.at[0]), pltpu.make_async_copy(w_down, w_down_in, w_sems.at[1]),
                     pltpu.make_async_copy(w_b, w_b_in, w_sems.at[2])]
    for copy in weight_copies:
        copy.start()

    barrier = pltpu.get_barrier_semaphore()
    for step in range(1, total):
        pl.semaphore_signal(barrier, inc=1, device_id=peer_of(step), device_id_type=MESH_ID)

    pos = lax.rem(lax.broadcasted_iota(jnp.int32, (block, LANES), 0), half)
    masks[0] = (pos != 0).astype(F32)
    masks[1] = (pos != half - 1).astype(F32)
    pixels[0:GUARD] = jnp.zeros((GUARD, LANES), F32)
    pixels[GUARD + n_img * width:] = jnp.zeros((GUARD, LANES), F32)

    def clear_guards(ref, outer):
        def body(idx, carry):
            view = ref.at[idx]
            view[0:GUARD] = jnp.zeros((GUARD, LANES), F32)
            view[GUARD + block:] = jnp.zeros((GUARD, LANES), F32)
            return carry
        lax.fori_loop(0, outer, body, 0)

    clear_guards(z_a, z_a.shape[0])
    clear_guards(z_mid, z_mid.shape[0])

    def clear_inner(ref):
        def body(idx, carry):
            view = ref.at[idx]
            view[0:GUARD] = jnp.zeros((GUARD, LANES), F32)
            view[GUARD + block:] = jnp.zeros((GUARD, LANES), F32)
            return carry
        lax.fori_loop(1, pairs + 1, body, 0)

    clear_inner(z_down)
    clear_inner(z_b)

    @pl.when(is_top)
    def _():
        x_in[:, 0:HALO] = jnp.zeros((n_img, HALO, width, x_in.shape[3]), BF16)
        z_down[0] = jnp.zeros(z_down.shape[1:], F32)
        z_b[0] = jnp.zeros(z_b.shape[1:], F32)

    @pl.when(is_bottom)
    def _():
        x_in[:, HALO + rows:] = jnp.zeros((n_img, HALO, width, x_in.shape[3]), BF16)
        z_down[pairs + 1] = jnp.zeros(z_down.shape[1:], F32)
        z_b[pairs + 1] = jnp.zeros(z_b.shape[1:], F32)

    def image_down():
        return pltpu.make_async_remote_copy(src_ref=images.at[:, pl.ds(rows - HALO, HALO)], dst_ref=x_in.at[:, pl.ds(0, HALO)],
                                            send_sem=image_send.at[0], recv_sem=image_recv.at[0],
                                            device_id={'sp': sp_idx + 1}, device_id_type=MESH_ID)

    def image_up():
        return pltpu.make_async_remote_copy(src_ref=images.at[:, pl.ds(0, HALO)], dst_ref=x_in.at[:, pl.ds(HALO + rows, HALO)],
                                            send_sem=image_send.at[1], recv_sem=image_recv.at[1],
                                            device_id={'sp': sp_idx - 1}, device_id_type=MESH_ID)

    def send_images():
        @pl.when(jnp.logical_not(is_bottom))
        def _():
            image_down().start()

        @pl.when(jnp.logical_not(is_top))
        def _():
            image_up().start()

    for copy in weight_copies:
        copy.wait()
    ch_a = w_a.shape[3]
    zero_a = jnp.zeros((ch_a, ch_a), BF16)
    zero_b = jnp.zeros((LANES, LANES), BF16)
    zero_d = jnp.zeros((ch_a, LANES), BF16)

    def tap_a(layer, p, q):
        return w_a_in[layer, p, q] if 0 <= p <= 2 and 0 <= q <= 2 else zero_a

    for layer in range(2):
        for q in range(4):
            for t in range(4):
                for dw in range(2):
                    both = jnp.concatenate([tap_a(layer, t, q - dw), tap_a(layer, t - 1, q - dw)], axis=1)
                    wide_a[layer, pl.ds((q * 4 + t) * ch_a, ch_a), pl.ds(dw * LANES, LANES)] = both
    for q in range(3):
        for t in range(6):
            for d in range(2):
                p = t - 1 - 2 * d
                wide_down[pl.ds((q * 6 + t) * ch_a, ch_a), pl.ds(d * LANES, LANES)] = w_down_in[p, q] if 0 <= p <= 2 else zero_d
    for layer in range(2):
        for q in range(3):
            for t in range(4):
                for d in range(2):
                    p = t - d
                    wide_b[layer, pl.ds((q * 4 + t) * LANES, LANES), pl.ds(d * LANES, LANES)] = w_b_in[layer, p, q] if 0 <= p <= 2 else zero_b

    def spread_pair(p):
        upper = x_in[:, 2 * p].astype(F32)
        lower = x_in[:, 2 * p + 1].astype(F32)
        both = jnp.concatenate([upper, lower], axis=2)
        pixels[pl.ds(GUARD, n_img * width)] = both.reshape(n_img * width, LANES)
        taps[0, p] = (pixels[pl.ds(GUARD - 1, block, stride=2)] * masks[0]).astype(BF16)
        taps[1, p] = pixels[pl.ds(GUARD, block, stride=2)].astype(BF16)
        taps[2, p] = pixels[pl.ds(GUARD + 1, block, stride=2)].astype(BF16)
        taps[3, p] = (pixels[pl.ds(GUARD + 2, block, stride=2)] * masks[1]).astype(BF16)

    def conv_a(layer, idx, dst):
        left = jnp.concatenate([taps[q, idx + s] for q in range(4) for s in range(2)], axis=1)
        z_val = jnp.dot(left, wide_a[layer], preferred_element_type=F32)
        dst[idx, pl.ds(GUARD, block)] = z_val[:, :LANES]
        dst[idx + dst.shape[0] // 2, pl.ds(GUARD, block)] = z_val[:, LANES:]
        return z_val

    def conv_down(idx):
        left = jnp.concatenate([taps[q, 2 * idx + s] for q in range(1, 4) for s in range(3)], axis=1)
        z_val = jnp.dot(left, wide_down[...], preferred_element_type=F32)
        z_down[2 * idx + 1, pl.ds(GUARD, block)] = z_val[:, :LANES]
        z_down[2 * idx + 2, pl.ds(GUARD, block)] = z_val[:, LANES:]
        return z_val

    def conv_b(layer, idx):
        left = jnp.concatenate([taps[q, 2 * idx + t] for q in range(3) for t in range(4)], axis=1)
        z_val = jnp.dot(left, wide_b[layer], preferred_element_type=F32)
        if layer == 0:
            z_b[2 * idx + 1, pl.ds(GUARD, block)] = z_val[:, :LANES]
            z_b[2 * idx + 2, pl.ds(GUARD, block)] = z_val[:, LANES:]
        else:
            z_last[pl.ds(2 * idx * last_stride, block)] = z_val[:, :LANES]
            z_last[pl.ds((2 * idx + 1) * last_stride, block)] = z_val[:, LANES:]
        return z_val

    def run(n_taps, first, per, n_conv, make_taps, conv, sums):
        made = 0

        def make_until(stop):
            nonlocal made
            while made < min(stop, n_taps):
                make_taps(made)
                made += 1

        for idx in range(n_conv):
            make_until(first + idx * per)
            sums = conv(idx, sums)
        return sums

    def add_sums(sums, z_val):
        tiles = z_val.reshape(block // 8, 8, 2 * LANES)
        return sums[0] + jnp.sum(tiles, axis=0), sums[1] + jnp.sum(tiles * tiles, axis=0)

    zero_sums = (jnp.zeros((8, 2 * LANES), F32), jnp.zeros((8, 2 * LANES), F32))

    def fold_sums(sums):
        rows_sum = [jnp.sum(val, axis=0, keepdims=True) for val in sums]
        return jnp.concatenate([val[:, :LANES] + val[:, LANES:] for val in rows_sum], axis=0)

    def sum_copy(layer, step):
        return pltpu.make_async_remote_copy(src_ref=parts.at[layer], dst_ref=slots.at[layer, me], send_sem=sum_send.at[layer],
                                            recv_sem=sum_recv.at[layer], device_id=peer_of(step), device_id_type=MESH_ID)

    def send_sums(layer, part):
        parts[layer] = part
        slots[layer, me] = part
        for step in range(1, total):
            sum_copy(layer, step).start()

    def group_sum(layer):
        others = slots.at[layer, pl.ds(0, total - 1)]
        pltpu.make_async_copy(others, others, sum_recv.at[layer]).wait()
        return jnp.sum(slots[layer], axis=0)

    def finish_sum(layer):
        others = slots.at[layer, pl.ds(0, total - 1)]
        pltpu.make_async_copy(others, others, sum_send.at[layer]).wait()

    def scales(sums, count, gamma, beta):
        mean = sums[0:1] / count
        var = sums[1:2] / count - mean * mean
        return mean, gamma * lax.rsqrt(var + EPS_VALUE), beta

    def scales_a(sums, count, pair):
        both = sums + jnp.concatenate([sums[:, LANES // 2:], sums[:, :LANES // 2]], axis=1)
        twice = jnp.concatenate([pair, pair], axis=1)
        return scales(both, count, twice[0:1], twice[1:2])

    def normed(z_val, scale, keep=None):
        mean, gain, beta = scale
        if keep is not None:
            gain, beta = gain * keep, beta * keep
        return jnp.maximum((z_val - mean) * gain + beta, 0.0)

    keep_top = jnp.where(is_top, 0.0, 1.0).astype(F32)
    keep_bottom = jnp.where(is_bottom, 0.0, 1.0).astype(F32)
    lane = lax.broadcasted_iota(jnp.int32, (1, LANES), 1)
    upper_half = (lane < LANES // 2).astype(F32)
    lower_half = 1.0 - upper_half

    for idx in range(n_chunk):
        image_copy(idx).wait()

    def conv_first(idx, acc):
        if idx == 2:
            pl.semaphore_wait(barrier, total - 1)
            send_images()
        return add_sums(acc, conv_a(0, 2 + idx, z_a))

    sums = run(pairs - 1, 2, 1, pairs - 2, lambda idx: spread_pair(2 + idx), conv_first, zero_sums)

    @pl.when(jnp.logical_not(is_top))
    def _():
        image_down().wait_recv()

    @pl.when(jnp.logical_not(is_bottom))
    def _():
        image_up().wait_recv()

    for idx in (0, 1, pairs + 1, pairs + 2):
        spread_pair(idx)
    for idx in (1, pairs):
        sums = add_sums(sums, conv_a(0, idx, z_a))
    send_sums(0, fold_sums(sums))
    for idx in (0, pairs + 1):
        conv_a(0, idx, z_a)
    count_a = n_img * rows * width * total
    scale = scales_a(group_sum(0), count_a, norm_a[0])

    def taps_mid(idx, src, scale, keep):
        odd = idx + src.shape[0] // 2
        taps[0, idx] = (normed(src[odd, pl.ds(GUARD - 1, block)], scale, keep) * masks[0]).astype(BF16)
        taps[1, idx] = normed(src[idx, pl.ds(GUARD, block)], scale, keep).astype(BF16)
        taps[2, idx] = normed(src[odd, pl.ds(GUARD, block)], scale, keep).astype(BF16)
        taps[3, idx] = (normed(src[idx, pl.ds(GUARD + 1, block)], scale, keep) * masks[1]).astype(BF16)

    def keep_pairs(idx):
        return keep_top if idx == 0 else keep_bottom if idx == pairs + 1 else None

    def conv_second(idx, acc):
        z_val = conv_a(1, idx, z_mid)
        if idx in (0, pairs):
            own = lower_half if idx == 0 else upper_half
            own = jnp.concatenate([own, own], axis=1)
            new = add_sums(zero_sums, z_val)
            return acc[0] + own * new[0], acc[1] + own * new[1]
        return add_sums(acc, z_val)

    sums = run(pairs + 2, 2, 1, pairs + 1, lambda idx: taps_mid(idx, z_a, scale, keep_pairs(idx)), conv_second, zero_sums)
    send_sums(1, fold_sums(sums))
    scale_mid = scales_a(group_sum(1), count_a, norm_a[1])

    def keep_staggered(idx):
        return upper_half + lower_half * keep_bottom if idx == pairs else None

    def conv_third(idx, acc):
        return add_sums(acc, conv_down(idx))

    sums = run(pairs + 1, 3, 2, pairs // 2, lambda idx: taps_mid(idx, z_mid, scale_mid, keep_staggered(idx)), conv_third, zero_sums)

    def edge_copies(ref, slot):
        below = pltpu.make_async_remote_copy(src_ref=ref.at[pairs], dst_ref=ref.at[0], send_sem=z_send.at[slot, 0], recv_sem=z_recv.at[slot, 0],
                                             device_id={'sp': sp_idx + 1}, device_id_type=MESH_ID)
        above = pltpu.make_async_remote_copy(src_ref=ref.at[1], dst_ref=ref.at[pairs + 1], send_sem=z_send.at[slot, 1], recv_sem=z_recv.at[slot, 1],
                                             device_id={'sp': sp_idx - 1}, device_id_type=MESH_ID)
        return below, above

    def send_edges(ref, slot):
        below, above = edge_copies(ref, slot)

        @pl.when(jnp.logical_not(is_bottom))
        def _():
            below.start()

        @pl.when(jnp.logical_not(is_top))
        def _():
            above.start()

    def recv_edges(ref, slot):
        below, above = edge_copies(ref, slot)

        @pl.when(jnp.logical_not(is_top))
        def _():
            below.wait_recv()

        @pl.when(jnp.logical_not(is_bottom))
        def _():
            above.wait_recv()

    def finish_edges(ref, slot):
        below, above = edge_copies(ref, slot)

        @pl.when(jnp.logical_not(is_bottom))
        def _():
            below.wait_send()

        @pl.when(jnp.logical_not(is_top))
        def _():
            above.wait_send()

    count_b = n_img * pairs * half * total
    send_sums(2, fold_sums(sums))
    send_edges(z_down, 0)
    scale_down = scales(group_sum(2), count_b, norm_down[0:1], norm_down[1:2])
    recv_edges(z_down, 0)

    def taps_low(idx, src, scale):
        keep = keep_pairs(idx)
        taps[0, idx] = (normed(src[idx, pl.ds(GUARD - 1, block)], scale, keep) * masks[0]).astype(BF16)
        taps[1, idx] = normed(src[idx, pl.ds(GUARD, block)], scale, keep).astype(BF16)
        taps[2, idx] = (normed(src[idx, pl.ds(GUARD + 1, block)], scale, keep) * masks[1]).astype(BF16)

    def conv_fourth(idx, acc):
        return add_sums(acc, conv_b(0, idx))

    def conv_fifth(idx, acc):
        return add_sums(acc, conv_b(1, idx))

    sums = run(pairs + 2, 4, 2, pairs // 2, lambda idx: taps_low(idx, z_down, scale_down), conv_fourth, zero_sums)
    send_sums(3, fold_sums(sums))
    send_edges(z_b, 1)
    scale_b = scales(group_sum(3), count_b, norm_b[0, 0:1], norm_b[0, 1:2])
    recv_edges(z_b, 1)
    sums = run(pairs + 2, 4, 2, pairs // 2, lambda idx: taps_low(idx, z_b, scale_b), conv_fifth, zero_sums)
    send_sums(4, fold_sums(sums))
    scale = scales(group_sum(4), count_b, norm_b[1, 0:1], norm_b[1, 1:2])

    n_out = out_sems.shape[0]
    out_chunk = n_img // n_out

    def out_copy(idx):
        return pltpu.make_async_copy(out_rows.at[pl.ds(idx * out_chunk, out_chunk)], out.at[pl.ds(idx * out_chunk, out_chunk)], out_sems.at[idx])

    def out_body(img, carry):
        for col in range(half):
            rows_val = z_last[pl.ds(img * half + col, pairs, stride=last_stride)]
            out_rows[img, col] = normed(rows_val, scale).astype(BF16)
        return carry

    for idx in range(n_out):
        lax.fori_loop(idx * out_chunk, (idx + 1) * out_chunk, out_body, 0)
        out_copy(idx).start()

    @pl.when(jnp.logical_not(is_bottom))
    def _():
        image_down().wait_send()

    @pl.when(jnp.logical_not(is_top))
    def _():
        image_up().wait_send()

    finish_edges(z_down, 0)
    finish_edges(z_b, 1)
    for layer in range(5):
        finish_sum(layer)
    for idx in range(n_out):
        out_copy(idx).wait()


def solution(mesh):
    group_size = mesh.shape['sp']
    data_size = mesh.shape['dp']
    total = data_size * group_size

    def local_stack(images, w_a, norm_a, w_down, norm_down, w_b, norm_b):
        n_img, rows, width, ch_a = images.shape
        ch_b = w_down.shape[3]
        pairs, half = rows // 2, width // 2
        block = n_img * half
        padded = block + 2 * GUARD
        any_spec = pl.BlockSpec(memory_space=pl.ANY)
        vmem_spec = pl.BlockSpec(memory_space=pltpu.VMEM)
        n_chunk, n_out = 4, 4
        result = pl.pallas_call(
            functools.partial(stack_kernel, data_size, group_size),
            out_shape=jax.ShapeDtypeStruct((n_img, half, pairs, ch_b), BF16),
            in_specs=[any_spec, any_spec, vmem_spec, any_spec, vmem_spec, any_spec, vmem_spec],
            out_specs=any_spec,
            scratch_shapes=[
                pltpu.VMEM((n_img, rows + 2 * HALO, width, ch_a), BF16),
                pltpu.VMEM(w_a.shape, BF16),
                pltpu.VMEM(w_down.shape, BF16),
                pltpu.VMEM(w_b.shape, BF16),
                pltpu.VMEM((2, 16 * ch_a, 2 * LANES), BF16),
                pltpu.VMEM((18 * ch_a, 2 * LANES), BF16),
                pltpu.VMEM((2, 12 * ch_b, 2 * LANES), BF16),
                pltpu.VMEM((n_img * width + 2 * GUARD, LANES), F32),
                pltpu.VMEM((2, block, LANES), F32),
                pltpu.VMEM((4, pairs + 3, block, LANES), BF16),
                pltpu.VMEM((2 * (pairs + 2), padded, LANES), F32),
                pltpu.VMEM((2 * (pairs + 1), padded, LANES), F32),
                pltpu.VMEM((pairs + 2, padded, LANES), F32),
                pltpu.VMEM((pairs + 2, padded, LANES), F32),
                pltpu.VMEM((pairs * (block + 1) + 7, LANES), F32),
                pltpu.VMEM((n_img, half, pairs, ch_b), BF16),
                pltpu.VMEM((5, 2, LANES), F32),
                pltpu.VMEM((5, total, 2, LANES), F32),
                pltpu.SemaphoreType.DMA((n_chunk,)),
                pltpu.SemaphoreType.DMA((3,)),
                pltpu.SemaphoreType.DMA((n_out,)),
                pltpu.SemaphoreType.DMA((2,)),
                pltpu.SemaphoreType.DMA((2,)),
                pltpu.SemaphoreType.DMA((2, 2)),
                pltpu.SemaphoreType.DMA((2, 2)),
                pltpu.SemaphoreType.DMA((5,)),
                pltpu.SemaphoreType.DMA((5,)),
            ],
            compiler_params=pltpu.CompilerParams(collective_id=0, has_side_effects=True, vmem_limit_bytes=60 * 1024 * 1024),
            name='conv_stack',
        )(images, w_a, norm_a, w_down, norm_down, w_b, norm_b)
        return jnp.transpose(result, (0, 2, 1, 3))

    act_spec = P(('pod', 'dp'), 'sp', None, None)
    return jax.shard_map(local_stack, mesh=mesh, in_specs=(act_spec, P(), P(), P(), P(), P(), P()), out_specs=act_spec, check_vma=False)
```

```python
import functools

import jax
import jax.numpy as jnp
from jax import lax
from jax.experimental import pallas as pl
from jax.experimental.pallas import tpu as pltpu
from jax.sharding import PartitionSpec as P

EPS_VALUE = 1e-5
MESH_ID = pl.DeviceIdType.MESH
LANES = 128
GUARD = 8
F32 = jnp.float32
BF16 = jnp.bfloat16


def stack_kernel(data_size, group_size, images, w_a, norm_a, w_down, norm_down, w_b, norm_b, z_out, mean_out, gain_out, beta_out,
                 x_in, w_a_in, w_down_in, w_b_in, norm_a_in, norm_down_in, norm_b_in, wide_a, wide_down, wide_b,
                 send_low, send_up, from_up, from_low, pixels, masks, taps, z_a, z_mid, z_down, z_b, z_last, z_turned, scale_rows,
                 parts, slots, in_sems, w_sems, out_sems, image_send, image_recv, z_send, z_recv, sum_send, sum_recv):
    n_img, rows, width, _ = images.shape
    half = width // 2
    last_stride = n_img * half + 1
    block = n_img * half
    pairs = rows // 2
    total = data_size * group_size
    dp_idx = lax.axis_index('dp')
    sp_idx = lax.axis_index('sp')
    me = dp_idx * group_size + sp_idx
    is_top = sp_idx == 0
    is_bottom = sp_idx == group_size - 1

    ring = group_size // 2

    def distance(peer):
        return min(peer[0], data_size - peer[0]) + min(peer[1], ring - peer[1])

    offsets = [(d, x, c) for d in range(data_size) for x in range(ring) for c in range(2)][1:]
    offsets.sort(key=distance, reverse=True)

    def peer_of(offset):
        core = lax.rem(sp_idx, 2)
        place = lax.rem(sp_idx // 2 + offset[1], ring)
        return {'dp': lax.rem(dp_idx + offset[0], data_size), 'sp': place * 2 + (1 - core if offset[2] else core)}

    n_chunk = in_sems.shape[0]
    chunk = rows // n_chunk

    def image_copy(idx):
        return pltpu.make_async_copy(images.at[:, pl.ds(idx * chunk, chunk)], x_in.at[:, pl.ds(idx * chunk, chunk)], in_sems.at[idx])

    for idx in [0, n_chunk - 1] + list(range(1, n_chunk - 1)):
        image_copy(idx).start()
    small_pairs = [(w_a, w_a_in), (norm_a, norm_a_in), (w_down, w_down_in), (norm_down, norm_down_in), (w_b, w_b_in), (norm_b, norm_b_in)]
    small_copies = [pltpu.make_async_copy(src, dst, w_sems.at[idx]) for idx, (src, dst) in enumerate(small_pairs)]
    for copy in small_copies:
        copy.start()

    barrier = pltpu.get_barrier_semaphore()
    for offset in offsets:
        pl.semaphore_signal(barrier, inc=1, device_id=peer_of(offset), device_id_type=MESH_ID)

    pos = lax.rem(lax.broadcasted_iota(jnp.int32, (block, LANES), 0), half)
    masks[0] = (pos != 0).astype(F32)
    masks[1] = (pos != half - 1).astype(F32)
    pixels[0:GUARD] = jnp.zeros((GUARD, LANES), F32)
    pixels[GUARD + n_img * width:] = jnp.zeros((GUARD, LANES), F32)

    def clear_guards(ref, outer):
        def body(idx, carry):
            view = ref.at[idx]
            view[0:GUARD] = jnp.zeros((GUARD, LANES), F32)
            view[GUARD + block:] = jnp.zeros((GUARD, LANES), F32)
            return carry
        lax.fori_loop(0, outer, body, 0)


    def clear_inner(ref):
        def body(idx, carry):
            view = ref.at[idx]
            view[0:GUARD] = jnp.zeros((GUARD, LANES), F32)
            view[GUARD + block:] = jnp.zeros((GUARD, LANES), F32)
            return carry
        lax.fori_loop(1, pairs + 1, body, 0)

    @pl.when(is_top)
    def _():
        from_up[...] = jnp.zeros(from_up.shape, BF16)
        z_down[0] = jnp.zeros(z_down.shape[1:], F32)
        z_b[0] = jnp.zeros(z_b.shape[1:], F32)

    @pl.when(is_bottom)
    def _():
        from_low[...] = jnp.zeros(from_low.shape, BF16)
        z_down[pairs + 1] = jnp.zeros(z_down.shape[1:], F32)
        z_b[pairs + 1] = jnp.zeros(z_b.shape[1:], F32)

    waited = set()

    def need_row(row):
        idx = row // chunk
        if idx not in waited:
            waited.add(idx)
            image_copy(idx).wait()

    for row in (0, rows - 1):
        need_row(row)
    plane = n_img * width

    def two_rows(row):
        return jnp.concatenate([x_in[:, row].astype(F32), x_in[:, row + 1].astype(F32)], axis=2).reshape(plane, LANES).astype(BF16)

    send_low[...] = two_rows(rows - 2)
    send_up[pl.ds(0, plane)] = two_rows(0)
    third = [x_in[pl.ds(idx * (n_img // 2), n_img // 2), 2].astype(F32) for idx in range(2)]
    send_up[pl.ds(plane, plane // 2)] = jnp.concatenate(third, axis=2).reshape(plane // 2, LANES).astype(BF16)

    def image_down():
        return pltpu.make_async_remote_copy(src_ref=send_low, dst_ref=from_up, send_sem=image_send.at[0], recv_sem=image_recv.at[0],
                                            device_id={'sp': sp_idx + 1}, device_id_type=MESH_ID)

    def image_up():
        return pltpu.make_async_remote_copy(src_ref=send_up, dst_ref=from_low, send_sem=image_send.at[1], recv_sem=image_recv.at[1],
                                            device_id={'sp': sp_idx - 1}, device_id_type=MESH_ID)

    def send_images():
        @pl.when(jnp.logical_not(is_bottom))
        def _():
            image_down().start()

        @pl.when(jnp.logical_not(is_top))
        def _():
            image_up().start()

    ch_a = w_a.shape[3]
    zero_a = jnp.zeros((ch_a, ch_a), BF16)
    zero_b = jnp.zeros((LANES, LANES), BF16)
    zero_d = jnp.zeros((ch_a, LANES), BF16)

    def tap_a(layer, p, q):
        return w_a_in[layer, p, q] if 0 <= p <= 2 and 0 <= q <= 2 else zero_a

    def widen_a(layer):
        for q in range(4):
            for t in range(4):
                for dw in range(2):
                    both = jnp.concatenate([tap_a(layer, t, q - dw), tap_a(layer, t - 1, q - dw)], axis=1)
                    wide_a[layer, pl.ds((q * 4 + t) * ch_a, ch_a), pl.ds(dw * LANES, LANES)] = both

    def widen_down():
        for q in range(3):
            for t in range(6):
                for d in range(2):
                    p = t - 1 - 2 * d
                    wide_down[pl.ds((q * 6 + t) * ch_a, ch_a), pl.ds(d * LANES, LANES)] = w_down_in[p, q] if 0 <= p <= 2 else zero_d

    def widen_b():
        for layer in range(2):
            for q in range(3):
                for t in range(4):
                    for d in range(2):
                        p = t - d
                        wide_b[layer, pl.ds((q * 4 + t) * LANES, LANES), pl.ds(d * LANES, LANES)] = w_b_in[layer, p, q] if 0 <= p <= 2 else zero_b

    def image_row(row):
        half_a = LANES // 2
        if row < -2:
            return jnp.zeros((plane, half_a), F32)
        if row < 0:
            return from_up[:, (row + 2) * half_a:(row + 3) * half_a].astype(F32)
        if row < rows:
            need_row(row)
            return x_in[:, row].astype(F32).reshape(plane, half_a)
        if row < rows + 2:
            return from_low[pl.ds(0, plane), (row - rows) * half_a:(row - rows + 1) * half_a].astype(F32)
        packed = from_low[pl.ds(plane, plane // 2), :].astype(F32)
        return jnp.concatenate([packed[:, :half_a], packed[:, half_a:]], axis=0)

    def spread_pair(p):
        both = jnp.concatenate([image_row(2 * p - 3), image_row(2 * p - 2)], axis=1)
        pixels[pl.ds(GUARD, n_img * width)] = both
        taps[0, p] = (pixels[pl.ds(GUARD - 1, block, stride=2)] * masks[0]).astype(BF16)
        taps[1, p] = pixels[pl.ds(GUARD, block, stride=2)].astype(BF16)
        taps[2, p] = pixels[pl.ds(GUARD + 1, block, stride=2)].astype(BF16)
        taps[3, p] = (pixels[pl.ds(GUARD + 2, block, stride=2)] * masks[1]).astype(BF16)

    def conv_a(layer, idx, dst):
        left = jnp.concatenate([taps[q, idx + s] for q in range(4) for s in range(2)], axis=1)
        z_val = jnp.dot(left, wide_a[layer], preferred_element_type=F32)
        dst[idx, pl.ds(GUARD, block)] = z_val[:, :LANES]
        dst[idx + dst.shape[0] // 2, pl.ds(GUARD, block)] = z_val[:, LANES:]
        return z_val

    def conv_down(idx):
        left = jnp.concatenate([taps[q, 2 * idx + s] for q in range(1, 4) for s in range(3)], axis=1)
        z_val = jnp.dot(left, wide_down[...], preferred_element_type=F32)
        z_down[2 * idx + 1, pl.ds(GUARD, block)] = z_val[:, :LANES]
        z_down[2 * idx + 2, pl.ds(GUARD, block)] = z_val[:, LANES:]
        return z_val

    def conv_b(layer, idx):
        left = jnp.concatenate([taps[q, 2 * idx + t] for q in range(3) for t in range(4)], axis=1)
        z_val = jnp.dot(left, wide_b[layer], preferred_element_type=F32)
        if layer == 0:
            z_b[2 * idx + 1, pl.ds(GUARD, block)] = z_val[:, :LANES]
            z_b[2 * idx + 2, pl.ds(GUARD, block)] = z_val[:, LANES:]
        else:
            z_last[pl.ds(2 * idx * last_stride, block)] = z_val[:, :LANES]
            z_last[pl.ds((2 * idx + 1) * last_stride, block)] = z_val[:, LANES:]
        return z_val

    def run(n_taps, first, per, n_conv, make_taps, conv, sums):
        made = 0

        def make_until(stop):
            nonlocal made
            while made < min(stop, n_taps):
                make_taps(made)
                made += 1

        for idx in range(n_conv):
            make_until(first + idx * per)
            sums = conv(idx, sums)
        return sums

    def add_sums(sums, z_val):
        tiles = z_val.reshape(block // 8, 8, 2 * LANES)
        return sums[0] + jnp.sum(tiles, axis=0), sums[1] + jnp.sum(tiles * tiles, axis=0)

    zero_sums = (jnp.zeros((8, 2 * LANES), F32), jnp.zeros((8, 2 * LANES), F32))

    def fold_sums(sums):
        rows_sum = [jnp.sum(val, axis=0, keepdims=True) for val in sums]
        return jnp.concatenate([val[:, :LANES] + val[:, LANES:] for val in rows_sum], axis=0)

    def sum_copy(layer, offset):
        return pltpu.make_async_remote_copy(src_ref=parts.at[layer], dst_ref=slots.at[layer, me], send_sem=sum_send.at[layer],
                                            recv_sem=sum_recv.at[layer], device_id=peer_of(offset), device_id_type=MESH_ID)

    def send_sums(layer, part):
        parts[layer] = part
        slots[layer, me] = part
        for offset in offsets:
            sum_copy(layer, offset).start()

    def group_sum(layer):
        others = slots.at[layer, pl.ds(0, total - 1)]
        pltpu.make_async_copy(others, others, sum_recv.at[layer]).wait()
        return jnp.sum(slots[layer], axis=0)

    def finish_sum(layer):
        others = slots.at[layer, pl.ds(0, total - 1)]
        pltpu.make_async_copy(others, others, sum_send.at[layer]).wait()

    def scales(sums, count, gamma, beta):
        mean = sums[0:1] / count
        var = sums[1:2] / count - mean * mean
        return mean, gamma * lax.rsqrt(var + EPS_VALUE), beta

    def scales_a(sums, count, pair):
        both = sums + jnp.concatenate([sums[:, LANES // 2:], sums[:, :LANES // 2]], axis=1)
        twice = jnp.concatenate([pair, pair], axis=1)
        return scales(both, count, twice[0:1], twice[1:2])

    def normed(z_val, scale, keep=None):
        mean, gain, beta = scale
        if keep is not None:
            gain, beta = gain * keep, beta * keep
        return jnp.maximum((z_val - mean) * gain + beta, 0.0)

    keep_top = jnp.where(is_top, 0.0, 1.0).astype(F32)
    keep_bottom = jnp.where(is_bottom, 0.0, 1.0).astype(F32)
    lane = lax.broadcasted_iota(jnp.int32, (1, LANES), 1)
    upper_half = (lane < LANES // 2).astype(F32)
    lower_half = 1.0 - upper_half

    small_copies[0].wait()
    widen_a(0)

    def conv_first(idx, acc):
        if idx == 1:
            pl.semaphore_wait(barrier, total - 1)
            send_images()
        return add_sums(acc, conv_a(0, 2 + idx, z_a))

    sums = run(pairs - 1, 2, 1, pairs - 2, lambda idx: spread_pair(2 + idx), conv_first, zero_sums)

    @pl.when(jnp.logical_not(is_top))
    def _():
        image_down().wait_recv()

    spread_pair(1)
    sums = add_sums(sums, conv_a(0, 1, z_a))

    @pl.when(jnp.logical_not(is_bottom))
    def _():
        image_up().wait_recv()

    spread_pair(pairs + 1)
    sums = add_sums(sums, conv_a(0, pairs, z_a))
    send_sums(0, fold_sums(sums))
    spread_pair(0)
    conv_a(0, 0, z_a)
    spread_pair(pairs + 2)
    conv_a(0, pairs + 1, z_a)
    for copy in small_copies[1:]:
        copy.wait()
    widen_a(1)
    widen_down()
    widen_b()
    clear_guards(z_a, z_a.shape[0])
    clear_guards(z_mid, z_mid.shape[0])
    clear_inner(z_down)
    clear_inner(z_b)
    count_a = n_img * rows * width * total
    scale = scales_a(group_sum(0), count_a, norm_a_in[0])

    def taps_mid(idx, src, scale, keep, left=True):
        odd = idx + src.shape[0] // 2
        if left:
            taps[0, idx] = (normed(src[odd, pl.ds(GUARD - 1, block)], scale, keep) * masks[0]).astype(BF16)
        taps[1, idx] = normed(src[idx, pl.ds(GUARD, block)], scale, keep).astype(BF16)
        taps[2, idx] = normed(src[odd, pl.ds(GUARD, block)], scale, keep).astype(BF16)
        taps[3, idx] = (normed(src[idx, pl.ds(GUARD + 1, block)], scale, keep) * masks[1]).astype(BF16)

    def keep_pairs(idx):
        return keep_top if idx == 0 else keep_bottom if idx == pairs + 1 else None

    def conv_second(idx, acc):
        z_val = conv_a(1, idx, z_mid)
        if idx in (0, pairs):
            own = lower_half if idx == 0 else upper_half
            own = jnp.concatenate([own, own], axis=1)
            new = add_sums(zero_sums, z_val)
            return acc[0] + own * new[0], acc[1] + own * new[1]
        return add_sums(acc, z_val)

    sums = run(pairs + 2, 2, 1, pairs + 1, lambda idx: taps_mid(idx, z_a, scale, keep_pairs(idx)), conv_second, zero_sums)
    send_sums(1, fold_sums(sums))
    scale_mid = scales_a(group_sum(1), count_a, norm_a_in[1])

    def keep_staggered(idx):
        return upper_half + lower_half * keep_bottom if idx == pairs else None

    def conv_third(idx, acc):
        return add_sums(acc, conv_down(idx))

    sums = run(pairs + 1, 3, 2, pairs // 2, lambda idx: taps_mid(idx, z_mid, scale_mid, keep_staggered(idx), left=False), conv_third, zero_sums)

    def edge_copies(ref, slot):
        below = pltpu.make_async_remote_copy(src_ref=ref.at[pairs], dst_ref=ref.at[0], send_sem=z_send.at[slot, 0], recv_sem=z_recv.at[slot, 0],
                                             device_id={'sp': sp_idx + 1}, device_id_type=MESH_ID)
        above = pltpu.make_async_remote_copy(src_ref=ref.at[1], dst_ref=ref.at[pairs + 1], send_sem=z_send.at[slot, 1], recv_sem=z_recv.at[slot, 1],
                                             device_id={'sp': sp_idx - 1}, device_id_type=MESH_ID)
        return below, above

    def send_edges(ref, slot):
        below, above = edge_copies(ref, slot)

        @pl.when(jnp.logical_not(is_bottom))
        def _():
            below.start()

        @pl.when(jnp.logical_not(is_top))
        def _():
            above.start()

    def recv_edges(ref, slot):
        below, above = edge_copies(ref, slot)

        @pl.when(jnp.logical_not(is_top))
        def _():
            below.wait_recv()

        @pl.when(jnp.logical_not(is_bottom))
        def _():
            above.wait_recv()

    def finish_edges(ref, slot):
        below, above = edge_copies(ref, slot)

        @pl.when(jnp.logical_not(is_bottom))
        def _():
            below.wait_send()

        @pl.when(jnp.logical_not(is_top))
        def _():
            above.wait_send()

    count_b = n_img * pairs * half * total
    send_sums(2, fold_sums(sums))
    send_edges(z_down, 0)
    scale_down = scales(group_sum(2), count_b, norm_down_in[0:1], norm_down_in[1:2])
    recv_edges(z_down, 0)

    def taps_low(idx, src, scale):
        keep = keep_pairs(idx)
        taps[0, idx] = (normed(src[idx, pl.ds(GUARD - 1, block)], scale, keep) * masks[0]).astype(BF16)
        taps[1, idx] = normed(src[idx, pl.ds(GUARD, block)], scale, keep).astype(BF16)
        taps[2, idx] = (normed(src[idx, pl.ds(GUARD + 1, block)], scale, keep) * masks[1]).astype(BF16)

    def conv_fourth(idx, acc):
        return add_sums(acc, conv_b(0, idx))

    def conv_fifth(idx, acc):
        return add_sums(acc, conv_b(1, idx))

    sums = run(pairs + 2, 4, 2, pairs // 2, lambda idx: taps_low(idx, z_down, scale_down), conv_fourth, zero_sums)
    send_sums(3, fold_sums(sums))
    send_edges(z_b, 1)
    scale_b = scales(group_sum(3), count_b, norm_b_in[0, 0:1], norm_b_in[0, 1:2])
    recv_edges(z_b, 1)
    sums = run(pairs + 2, 4, 2, pairs // 2, lambda idx: taps_low(idx, z_b, scale_b), conv_fifth, zero_sums)
    send_sums(4, fold_sums(sums))

    n_out = out_sems.shape[0] - 3
    out_chunk = n_img // n_out

    def out_copy(idx):
        part = pl.ds(idx * out_chunk, out_chunk)
        return pltpu.make_async_copy(z_turned.at[part], z_out.at[part], out_sems.at[idx])

    def turn(img, carry):
        for col in range(half):
            z_turned[img, col] = z_last[pl.ds(img * half + col, pairs, stride=last_stride)]
        return carry

    for idx in range(n_out):
        lax.fori_loop(idx * out_chunk, (idx + 1) * out_chunk, turn, 0)
        out_copy(idx).start()
    mean, gain, beta = scales(group_sum(4), count_b, norm_b_in[1, 0:1], norm_b_in[1, 1:2])
    scale_copies = []
    for idx, (val, dst) in enumerate([(mean, mean_out), (gain, gain_out), (beta, beta_out)]):
        scale_rows[idx] = val
        scale_copies.append(pltpu.make_async_copy(scale_rows.at[idx], dst, out_sems.at[n_out + idx]))
    for copy in scale_copies:
        copy.start()

    @pl.when(jnp.logical_not(is_bottom))
    def _():
        image_down().wait_send()

    @pl.when(jnp.logical_not(is_top))
    def _():
        image_up().wait_send()

    finish_edges(z_down, 0)
    finish_edges(z_b, 1)
    for layer in range(5):
        finish_sum(layer)
    for idx in range(n_out):
        out_copy(idx).wait()
    for copy in scale_copies:
        copy.wait()


def solution(mesh):
    group_size = mesh.shape['sp']
    data_size = mesh.shape['dp']
    total = data_size * group_size

    def local_stack(images, w_a, norm_a, w_down, norm_down, w_b, norm_b):
        n_img, rows, width, ch_a = images.shape
        ch_b = w_down.shape[3]
        pairs, half = rows // 2, width // 2
        block = n_img * half
        padded = block + 2 * GUARD
        any_spec = pl.BlockSpec(memory_space=pl.ANY)
        n_chunk, n_out = 8, 4
        z_val, mean, gain, beta = pl.pallas_call(
            functools.partial(stack_kernel, data_size, group_size),
            out_shape=(jax.ShapeDtypeStruct((n_img, half, pairs, ch_b), F32),) + (jax.ShapeDtypeStruct((1, LANES), F32),) * 3,
            in_specs=[any_spec] * 7,
            out_specs=(any_spec,) * 4,
            scratch_shapes=[
                pltpu.VMEM((n_img, rows, width, ch_a), BF16),
                pltpu.VMEM(w_a.shape, BF16),
                pltpu.VMEM(w_down.shape, BF16),
                pltpu.VMEM(w_b.shape, BF16),
                pltpu.VMEM(norm_a.shape, F32),
                pltpu.VMEM(norm_down.shape, F32),
                pltpu.VMEM(norm_b.shape, F32),
                pltpu.VMEM((2, 16 * ch_a, 2 * LANES), BF16),
                pltpu.VMEM((18 * ch_a, 2 * LANES), BF16),
                pltpu.VMEM((2, 12 * ch_b, 2 * LANES), BF16),
                pltpu.VMEM((n_img * width, LANES), BF16),
                pltpu.VMEM((n_img * width * 3 // 2, LANES), BF16),
                pltpu.VMEM((n_img * width, LANES), BF16),
                pltpu.VMEM((n_img * width * 3 // 2, LANES), BF16),
                pltpu.VMEM((n_img * width + 2 * GUARD, LANES), F32),
                pltpu.VMEM((2, block, LANES), F32),
                pltpu.VMEM((4, pairs + 3, block, LANES), BF16),
                pltpu.VMEM((2 * (pairs + 2), padded, LANES), F32),
                pltpu.VMEM((2 * (pairs + 1), padded, LANES), F32),
                pltpu.VMEM((pairs + 2, padded, LANES), F32),
                pltpu.VMEM((pairs + 2, padded, LANES), F32),
                pltpu.VMEM((pairs * (block + 1) + 7, LANES), F32),
                pltpu.VMEM((n_img, half, pairs, ch_b), F32),
                pltpu.VMEM((3, 1, LANES), F32),
                pltpu.VMEM((5, 2, LANES), F32),
                pltpu.VMEM((5, total, 2, LANES), F32),
                pltpu.SemaphoreType.DMA((n_chunk,)),
                pltpu.SemaphoreType.DMA((6,)),
                pltpu.SemaphoreType.DMA((n_out + 3,)),
                pltpu.SemaphoreType.DMA((2,)),
                pltpu.SemaphoreType.DMA((2,)),
                pltpu.SemaphoreType.DMA((2, 2)),
                pltpu.SemaphoreType.DMA((2, 2)),
                pltpu.SemaphoreType.DMA((5,)),
                pltpu.SemaphoreType.DMA((5,)),
            ],
            compiler_params=pltpu.CompilerParams(collective_id=0, has_side_effects=True, vmem_limit_bytes=60 * 1024 * 1024),
            name='conv_stack',
        )(images, w_a, norm_a, w_down, norm_down, w_b, norm_b)
        result = jnp.maximum((z_val - mean[0]) * gain[0] + beta[0], 0.0).astype(BF16)
        return jnp.transpose(result, (0, 2, 1, 3))

    act_spec = P(('pod', 'dp'), 'sp', None, None)
    return jax.shard_map(local_stack, mesh=mesh, in_specs=(act_spec, P(), P(), P(), P(), P(), P()), out_specs=act_spec, check_vma=False)
```

```python
import functools

import jax
import jax.numpy as jnp
from jax import lax
from jax.experimental import pallas as pl
from jax.experimental.pallas import tpu as pltpu
from jax.sharding import PartitionSpec as P

EPS_VALUE = 1e-5
MESH_ID = pl.DeviceIdType.MESH
LANES = 128
GUARD = 8
F32 = jnp.float32
BF16 = jnp.bfloat16


def stack_kernel(data_size, group_size, images, w_a, norm_a, w_down, norm_down, w_b, norm_b, z_out, mean_out, gain_out, beta_out,
                 x_in, w_a_in, w_down_in, w_b_in, norm_a_in, norm_down_in, norm_b_in, wide_a, wide_down, wide_b,
                 send_low, send_up, from_up, from_low, pixels, masks, taps, z_a, z_mid, z_down, z_b, z_last, z_turned, scale_rows,
                 parts, slots, in_sems, w_sems, out_sems, image_send, image_recv, z_send, z_recv, sum_send, sum_recv):
    n_img, rows, width, _ = images.shape
    half = width // 2
    last_stride = n_img * half + 1
    block = n_img * half
    pairs = rows // 2
    total = data_size * group_size
    dp_idx = lax.axis_index('dp')
    sp_idx = lax.axis_index('sp')
    me = dp_idx * group_size + sp_idx
    is_top = sp_idx == 0
    is_bottom = sp_idx == group_size - 1
    keep_top = jnp.where(is_top, 0.0, 1.0).astype(F32)
    keep_bottom = jnp.where(is_bottom, 0.0, 1.0).astype(F32)

    ring = group_size // 2

    def distance(peer):
        return min(peer[0], data_size - peer[0]) + min(peer[1], ring - peer[1])

    offsets = [(d, x, c) for d in range(data_size) for x in range(ring) for c in range(2)][1:]
    offsets.sort(key=distance, reverse=True)

    def peer_of(offset):
        core = lax.rem(sp_idx, 2)
        place = lax.rem(sp_idx // 2 + offset[1], ring)
        return {'dp': lax.rem(dp_idx + offset[0], data_size), 'sp': place * 2 + (1 - core if offset[2] else core)}

    n_chunk = in_sems.shape[0]
    chunk = rows // n_chunk

    def image_copy(idx):
        return pltpu.make_async_copy(images.at[:, pl.ds(idx * chunk, chunk)], x_in.at[:, pl.ds(idx * chunk, chunk)], in_sems.at[idx])

    image_copy(0).start()
    image_copy(n_chunk - 1).start()
    barrier = pltpu.get_barrier_semaphore()
    for offset in offsets:
        pl.semaphore_signal(barrier, inc=1, device_id=peer_of(offset), device_id_type=MESH_ID)
    for idx in range(1, n_chunk - 1):
        image_copy(idx).start()
    small_pairs = [(w_a, w_a_in), (norm_a, norm_a_in), (w_down, w_down_in), (norm_down, norm_down_in), (w_b, w_b_in), (norm_b, norm_b_in)]
    small_copies = [pltpu.make_async_copy(src, dst, w_sems.at[idx]) for idx, (src, dst) in enumerate(small_pairs)]
    for copy in small_copies:
        copy.start()

    pos = lax.rem(lax.broadcasted_iota(jnp.int32, (block, LANES), 0), half)
    masks[0] = (pos != 0).astype(F32)
    masks[1] = (pos != half - 1).astype(F32)
    pixels[0:GUARD] = jnp.zeros((GUARD, LANES), F32)
    pixels[GUARD + n_img * width:] = jnp.zeros((GUARD, LANES), F32)

    def clear_guards(ref, outer):
        def body(idx, carry):
            view = ref.at[idx]
            view[0:GUARD] = jnp.zeros((GUARD, LANES), F32)
            view[GUARD + block:] = jnp.zeros((GUARD, LANES), F32)
            return carry
        lax.fori_loop(0, outer, body, 0)


    def clear_inner(ref):
        def body(idx, carry):
            view = ref.at[idx]
            view[0:GUARD] = jnp.zeros((GUARD, LANES), F32)
            view[GUARD + block:] = jnp.zeros((GUARD, LANES), F32)
            return carry
        lax.fori_loop(1, pairs + 1, body, 0)

    @pl.when(is_top)
    def _():
        from_up[...] = jnp.zeros(from_up.shape, BF16)

    @pl.when(is_bottom)
    def _():
        from_low[...] = jnp.zeros(from_low.shape, BF16)

    waited = set()

    def need_row(row):
        idx = row // chunk
        if idx not in waited:
            waited.add(idx)
            image_copy(idx).wait()

    for row in (0, rows - 1):
        need_row(row)
    plane = n_img * width

    def packed_row(row):
        halves = [x_in[pl.ds(idx * (n_img // 2), n_img // 2), row].astype(F32) for idx in range(2)]
        return jnp.concatenate(halves, axis=2).reshape(plane // 2, LANES).astype(BF16)

    for idx in range(2):
        send_low[idx] = packed_row(rows - 1 - idx)
    for idx in range(3):
        send_up[idx] = packed_row(idx)

    def image_copies(down, part):
        src, dst = (send_low, from_up) if down else (send_up, from_low)
        span = pl.ds(0, 1) if part == 0 else pl.ds(1, src.shape[0] - 1)
        place = 2 * part + (0 if down else 1)
        return pltpu.make_async_remote_copy(src_ref=src.at[span], dst_ref=dst.at[span], send_sem=image_send.at[place], recv_sem=image_recv.at[place],
                                            device_id={'sp': sp_idx + 1 if down else sp_idx - 1}, device_id_type=MESH_ID)

    def send_images():
        @pl.when(jnp.logical_not(is_bottom))
        def _():
            image_copies(True, 0).start()
            image_copies(True, 1).start()

        @pl.when(jnp.logical_not(is_top))
        def _():
            image_copies(False, 0).start()
            image_copies(False, 1).start()

    def recv_images(part):
        @pl.when(jnp.logical_not(is_top))
        def _():
            image_copies(True, part).wait_recv()

        @pl.when(jnp.logical_not(is_bottom))
        def _():
            image_copies(False, part).wait_recv()

    def finish_images():
        @pl.when(jnp.logical_not(is_bottom))
        def _():
            image_copies(True, 0).wait_send()
            image_copies(True, 1).wait_send()

        @pl.when(jnp.logical_not(is_top))
        def _():
            image_copies(False, 0).wait_send()
            image_copies(False, 1).wait_send()

    ch_a = w_a.shape[3]
    zero_a = jnp.zeros((ch_a, ch_a), BF16)
    zero_b = jnp.zeros((LANES, LANES), BF16)
    zero_d = jnp.zeros((ch_a, LANES), BF16)

    def tap_a(layer, p, q):
        return w_a_in[layer, p, q] if 0 <= p <= 2 and 0 <= q <= 2 else zero_a

    def widen_a(layer):
        for q in range(4):
            for t in range(4):
                for dw in range(2):
                    both = jnp.concatenate([tap_a(layer, t, q - dw), tap_a(layer, t - 1, q - dw)], axis=1)
                    wide_a[layer, pl.ds((q * 4 + t) * ch_a, ch_a), pl.ds(dw * LANES, LANES)] = both

    def widen_down():
        for q in range(3):
            for t in range(6):
                for d in range(2):
                    p = t - 1 - 2 * d
                    wide_down[pl.ds((q * 6 + t) * ch_a, ch_a), pl.ds(d * LANES, LANES)] = w_down_in[p, q] if 0 <= p <= 2 else zero_d

    def widen_b():
        for layer in range(2):
            for q in range(3):
                for t in range(4):
                    for d in range(2):
                        p = t - d
                        wide_b[layer, pl.ds((q * 4 + t) * LANES, LANES), pl.ds(d * LANES, LANES)] = w_b_in[layer, p, q] if 0 <= p <= 2 else zero_b

    def image_row(row):
        half_a = LANES // 2
        if row < -2:
            return jnp.zeros((plane, half_a), F32)
        if 0 <= row < rows:
            need_row(row)
            return x_in[:, row].astype(F32).reshape(plane, half_a)
        packed = (from_up[-1 - row] if row < 0 else from_low[row - rows]).astype(F32)
        return jnp.concatenate([packed[:, :half_a], packed[:, half_a:]], axis=0)

    def spread_pair(p):
        both = jnp.concatenate([image_row(2 * p - 3), image_row(2 * p - 2)], axis=1)
        pixels[pl.ds(GUARD, n_img * width)] = both
        taps[0, p] = (pixels[pl.ds(GUARD - 1, block, stride=2)] * masks[0]).astype(BF16)
        taps[1, p] = pixels[pl.ds(GUARD, block, stride=2)].astype(BF16)
        taps[2, p] = pixels[pl.ds(GUARD + 1, block, stride=2)].astype(BF16)
        taps[3, p] = (pixels[pl.ds(GUARD + 2, block, stride=2)] * masks[1]).astype(BF16)

    def conv_a(layer, idx, dst):
        left = jnp.concatenate([taps[q, idx + s] for q in range(4) for s in range(2)], axis=1)
        z_val = jnp.dot(left, wide_a[layer], preferred_element_type=F32)
        dst[idx, pl.ds(GUARD, block)] = z_val[:, :LANES]
        dst[idx + dst.shape[0] // 2, pl.ds(GUARD, block)] = z_val[:, LANES:]
        return z_val

    def conv_down(idx):
        left = jnp.concatenate([taps[q, 2 * idx + s] for q in range(1, 4) for s in range(3)], axis=1)
        z_val = jnp.dot(left, wide_down[...], preferred_element_type=F32)
        z_down[2 * idx + 1, pl.ds(GUARD, block)] = z_val[:, :LANES]
        z_down[2 * idx + 2, pl.ds(GUARD, block)] = z_val[:, LANES:]
        return z_val

    def conv_b(layer, idx):
        left = jnp.concatenate([taps[q, 2 * idx + t] for q in range(3) for t in range(4)], axis=1)
        z_val = jnp.dot(left, wide_b[layer], preferred_element_type=F32)
        if layer == 0:
            z_b[2 * idx + 1, pl.ds(GUARD, block)] = z_val[:, :LANES]
            z_b[2 * idx + 2, pl.ds(GUARD, block)] = z_val[:, LANES:]
        else:
            z_last[pl.ds(2 * idx * last_stride, block)] = z_val[:, :LANES]
            z_last[pl.ds((2 * idx + 1) * last_stride, block)] = z_val[:, LANES:]
        return z_val

    def run(tap_order, conv_order, need, make_taps, conv, sums):
        made = 0
        for idx, count in zip(conv_order, need):
            for tap in tap_order[made:count]:
                make_taps(tap)
            made = max(made, count)
            sums = conv(idx, sums)
        return sums

    def add_sums(sums, z_val):
        tiles = z_val.reshape(block // 8, 8, 2 * LANES)
        return sums[0] + jnp.sum(tiles, axis=0), sums[1] + jnp.sum(tiles * tiles, axis=0)

    zero_sums = (jnp.zeros((8, 2 * LANES), F32), jnp.zeros((8, 2 * LANES), F32))

    def fold_sums(sums):
        rows_sum = [jnp.sum(val, axis=0, keepdims=True) for val in sums]
        return jnp.concatenate([val[:, :LANES] + val[:, LANES:] for val in rows_sum], axis=0)

    def sum_copy(layer, offset):
        return pltpu.make_async_remote_copy(src_ref=parts.at[layer], dst_ref=slots.at[layer, me], send_sem=sum_send.at[layer],
                                            recv_sem=sum_recv.at[layer], device_id=peer_of(offset), device_id_type=MESH_ID)

    def send_sums(layer, part):
        parts[layer] = part
        slots[layer, me] = part
        for offset in offsets:
            sum_copy(layer, offset).start()

    def group_sum(layer):
        others = slots.at[layer, pl.ds(0, total - 1)]
        pltpu.make_async_copy(others, others, sum_recv.at[layer]).wait()
        return jnp.sum(slots[layer], axis=0)

    def finish_sum(layer):
        others = slots.at[layer, pl.ds(0, total - 1)]
        pltpu.make_async_copy(others, others, sum_send.at[layer]).wait()

    def scales(sums, count, gamma, beta):
        mean = sums[0:1] / count
        var = sums[1:2] / count - mean * mean
        return mean, gamma * lax.rsqrt(var + EPS_VALUE), beta

    def scales_a(sums, count, pair):
        both = sums + jnp.concatenate([sums[:, LANES // 2:], sums[:, :LANES // 2]], axis=1)
        twice = jnp.concatenate([pair, pair], axis=1)
        return scales(both, count, twice[0:1], twice[1:2])

    def normed(z_val, scale, keep=None):
        mean, gain, beta = scale
        if keep is not None:
            gain, beta = gain * keep, beta * keep
        return jnp.maximum((z_val - mean) * gain + beta, 0.0)

    lane = lax.broadcasted_iota(jnp.int32, (1, LANES), 1)
    upper_half = (lane < LANES // 2).astype(F32)
    lower_half = 1.0 - upper_half

    small_copies[0].wait()
    widen_a(0)

    def conv_first(idx, acc):
        return add_sums(acc, conv_a(0, idx, z_a))

    early = (3 * chunk + 1) // 2
    for row in (chunk, 2 * chunk):
        need_row(row)
    sums = run(range(2, early + 1), range(2, early), range(2, early), spread_pair, conv_first, zero_sums)
    pl.semaphore_wait(barrier, total - 1)
    send_images()
    for row in range(0, rows, chunk):
        need_row(row)
    last = pairs - 2
    sums = run(range(early + 1, last + 3), range(early, last + 2), range(1, last - early + 3), spread_pair, conv_first, sums)
    recv_images(0)
    sums = run([1, pairs + 1], [1, pairs], [1, 2], spread_pair, conv_first, sums)
    send_sums(0, fold_sums(sums))
    recv_images(1)
    spread_pair(0)
    conv_a(0, 0, z_a)
    spread_pair(pairs + 2)
    conv_a(0, pairs + 1, z_a)
    for copy in small_copies[1:]:
        copy.wait()
    widen_a(1)
    widen_down()
    widen_b()
    clear_guards(z_a, z_a.shape[0])
    clear_guards(z_mid, z_mid.shape[0])
    clear_inner(z_down)
    clear_inner(z_b)
    count_a = n_img * rows * width * total
    scale = scales_a(group_sum(0), count_a, norm_a_in[0])

    def taps_mid(idx, src, scale, keep, left=True):
        odd = idx + src.shape[0] // 2
        if left:
            taps[0, idx] = (normed(src[odd, pl.ds(GUARD - 1, block)], scale, keep) * masks[0]).astype(BF16)
        taps[1, idx] = normed(src[idx, pl.ds(GUARD, block)], scale, keep).astype(BF16)
        taps[2, idx] = normed(src[odd, pl.ds(GUARD, block)], scale, keep).astype(BF16)
        taps[3, idx] = (normed(src[idx, pl.ds(GUARD + 1, block)], scale, keep) * masks[1]).astype(BF16)

    def keep_pairs(idx):
        return keep_top if idx == 0 else keep_bottom if idx == pairs + 1 else None

    def conv_second(idx, acc):
        z_val = conv_a(1, idx, z_mid)
        if idx in (0, pairs):
            own = lower_half if idx == 0 else upper_half
            own = jnp.concatenate([own, own], axis=1)
            new = add_sums(zero_sums, z_val)
            return acc[0] + own * new[0], acc[1] + own * new[1]
        return add_sums(acc, z_val)

    sums = run(range(pairs + 2), range(pairs + 1), range(2, pairs + 3), lambda idx: taps_mid(idx, z_a, scale, keep_pairs(idx)), conv_second, zero_sums)
    send_sums(1, fold_sums(sums))
    scale_mid = scales_a(group_sum(1), count_a, norm_a_in[1])

    def keep_staggered(idx):
        return upper_half + lower_half * keep_bottom if idx == pairs else None

    def edge_copies(ref, slot):
        below = pltpu.make_async_remote_copy(src_ref=ref.at[pairs], dst_ref=ref.at[0], send_sem=z_send.at[slot, 0], recv_sem=z_recv.at[slot, 0],
                                             device_id={'sp': lax.rem(sp_idx + 1, group_size)}, device_id_type=MESH_ID)
        above = pltpu.make_async_remote_copy(src_ref=ref.at[1], dst_ref=ref.at[pairs + 1], send_sem=z_send.at[slot, 1], recv_sem=z_recv.at[slot, 1],
                                             device_id={'sp': lax.rem(sp_idx + group_size - 1, group_size)}, device_id_type=MESH_ID)
        return below, above

    def send_edges(ref, slot):
        for copy in edge_copies(ref, slot):
            copy.start()

    def recv_edges(ref, slot):
        for copy in edge_copies(ref, slot):
            copy.wait_recv()

    def finish_edges(ref, slot):
        for copy in edge_copies(ref, slot):
            copy.wait_send()

    count_b = n_img * pairs * half * total
    last = pairs // 2 - 1
    def conv_third(idx, acc):
        return add_sums(acc, conv_down(idx))

    sums = run(range(pairs + 1), range(last + 1), range(3, pairs + 2, 2), lambda idx: taps_mid(idx, z_mid, scale_mid, keep_staggered(idx), left=False), conv_third, zero_sums)
    send_sums(2, fold_sums(sums))
    send_edges(z_down, 0)
    scale_down = scales(group_sum(2), count_b, norm_down_in[0:1], norm_down_in[1:2])
    recv_edges(z_down, 0)

    def taps_low(idx, src, scale):
        keep = keep_pairs(idx)
        taps[0, idx] = (normed(src[idx, pl.ds(GUARD - 1, block)], scale, keep) * masks[0]).astype(BF16)
        taps[1, idx] = normed(src[idx, pl.ds(GUARD, block)], scale, keep).astype(BF16)
        taps[2, idx] = (normed(src[idx, pl.ds(GUARD + 1, block)], scale, keep) * masks[1]).astype(BF16)

    def conv_fourth(idx, acc):
        return add_sums(acc, conv_b(0, idx))

    def conv_fifth(idx, acc):
        return add_sums(acc, conv_b(1, idx))

    sums = run(range(pairs + 2), range(last + 1), range(4, pairs + 3, 2), lambda idx: taps_low(idx, z_down, scale_down), conv_fourth, zero_sums)
    send_sums(3, fold_sums(sums))
    send_edges(z_b, 1)
    scale_b = scales(group_sum(3), count_b, norm_b_in[0, 0:1], norm_b_in[0, 1:2])
    recv_edges(z_b, 1)
    sums = run(range(pairs + 2), range(last + 1), range(4, pairs + 3, 2), lambda idx: taps_low(idx, z_b, scale_b), conv_fifth, zero_sums)
    send_sums(4, fold_sums(sums))

    n_out = out_sems.shape[0] - 3
    out_chunk = n_img // n_out

    def out_copy(idx):
        part = pl.ds(idx * out_chunk, out_chunk)
        return pltpu.make_async_copy(z_turned.at[part], z_out.at[part], out_sems.at[idx])

    def turn(img, carry):
        for col in range(half):
            z_turned[img, col] = z_last[pl.ds(img * half + col, pairs, stride=last_stride)]
        return carry

    for idx in range(n_out):
        lax.fori_loop(idx * out_chunk, (idx + 1) * out_chunk, turn, 0)
        out_copy(idx).start()
    mean, gain, beta = scales(group_sum(4), count_b, norm_b_in[1, 0:1], norm_b_in[1, 1:2])
    scale_copies = []
    for idx, (val, dst) in enumerate([(mean, mean_out), (gain, gain_out), (beta, beta_out)]):
        scale_rows[idx] = val
        scale_copies.append(pltpu.make_async_copy(scale_rows.at[idx], dst, out_sems.at[n_out + idx]))
    for copy in scale_copies:
        copy.start()

    finish_images()
    finish_edges(z_down, 0)
    finish_edges(z_b, 1)
    for layer in range(5):
        finish_sum(layer)
    for idx in range(n_out):
        out_copy(idx).wait()
    for copy in scale_copies:
        copy.wait()


def norm_kernel(z_hbm, mean_hbm, gain_hbm, beta_hbm, out_hbm, z_ref, rows_ref, out_ref, z_sems, row_sems, out_sems):
    n_step = z_sems.shape[0]
    size = z_ref.shape[0] // n_step
    row_copies = [pltpu.make_async_copy(src, rows_ref.at[idx], row_sems.at[idx]) for idx, src in enumerate((mean_hbm, gain_hbm, beta_hbm))]
    parts = [pl.ds(idx * size, size) for idx in range(n_step)]
    z_copies = [pltpu.make_async_copy(z_hbm.at[part], z_ref.at[part], z_sems.at[idx]) for idx, part in enumerate(parts)]
    out_copies = [pltpu.make_async_copy(out_ref.at[part], out_hbm.at[part], out_sems.at[idx]) for idx, part in enumerate(parts)]
    for copy in row_copies + z_copies:
        copy.start()
    for copy in row_copies:
        copy.wait()
    for part, z_copy, out_copy in zip(parts, z_copies, out_copies):
        z_copy.wait()
        out_ref[part] = jnp.maximum((z_ref[part] - rows_ref[0]) * rows_ref[1] + rows_ref[2], 0.0).astype(BF16)
        out_copy.start()
    for copy in out_copies:
        copy.wait()


def solution(mesh):
    group_size = mesh.shape['sp']
    data_size = mesh.shape['dp']
    total = data_size * group_size

    def local_stack(images, w_a, norm_a, w_down, norm_down, w_b, norm_b):
        n_img, rows, width, ch_a = images.shape
        ch_b = w_down.shape[3]
        pairs, half = rows // 2, width // 2
        block = n_img * half
        padded = block + 2 * GUARD
        any_spec = pl.BlockSpec(memory_space=pl.ANY)
        n_chunk, n_out = 8, 4
        z_val, mean, gain, beta = pl.pallas_call(
            functools.partial(stack_kernel, data_size, group_size),
            out_shape=(jax.ShapeDtypeStruct((n_img, half, pairs, ch_b), F32),) + (jax.ShapeDtypeStruct((1, LANES), F32),) * 3,
            in_specs=[any_spec] * 7,
            out_specs=(any_spec,) * 4,
            scratch_shapes=[
                pltpu.VMEM((n_img, rows, width, ch_a), BF16),
                pltpu.VMEM(w_a.shape, BF16),
                pltpu.VMEM(w_down.shape, BF16),
                pltpu.VMEM(w_b.shape, BF16),
                pltpu.VMEM(norm_a.shape, F32),
                pltpu.VMEM(norm_down.shape, F32),
                pltpu.VMEM(norm_b.shape, F32),
                pltpu.VMEM((2, 16 * ch_a, 2 * LANES), BF16),
                pltpu.VMEM((18 * ch_a, 2 * LANES), BF16),
                pltpu.VMEM((2, 12 * ch_b, 2 * LANES), BF16),
                pltpu.VMEM((2, n_img * width // 2, LANES), BF16),
                pltpu.VMEM((3, n_img * width // 2, LANES), BF16),
                pltpu.VMEM((2, n_img * width // 2, LANES), BF16),
                pltpu.VMEM((3, n_img * width // 2, LANES), BF16),
                pltpu.VMEM((n_img * width + 2 * GUARD, LANES), F32),
                pltpu.VMEM((2, block, LANES), F32),
                pltpu.VMEM((4, pairs + 3, block, LANES), BF16),
                pltpu.VMEM((2 * (pairs + 2), padded, LANES), F32),
                pltpu.VMEM((2 * (pairs + 1), padded, LANES), F32),
                pltpu.VMEM((pairs + 2, padded, LANES), F32),
                pltpu.VMEM((pairs + 2, padded, LANES), F32),
                pltpu.VMEM((pairs * (block + 1) + 7, LANES), F32),
                pltpu.VMEM((n_img, half, pairs, ch_b), F32),
                pltpu.VMEM((3, 1, LANES), F32),
                pltpu.VMEM((5, 2, LANES), F32),
                pltpu.VMEM((5, total, 2, LANES), F32),
                pltpu.SemaphoreType.DMA((n_chunk,)),
                pltpu.SemaphoreType.DMA((6,)),
                pltpu.SemaphoreType.DMA((n_out + 3,)),
                pltpu.SemaphoreType.DMA((4,)),
                pltpu.SemaphoreType.DMA((4,)),
                pltpu.SemaphoreType.DMA((2, 2)),
                pltpu.SemaphoreType.DMA((2, 2)),
                pltpu.SemaphoreType.DMA((5,)),
                pltpu.SemaphoreType.DMA((5,)),
            ],
            compiler_params=pltpu.CompilerParams(collective_id=0, has_side_effects=True, vmem_limit_bytes=60 * 1024 * 1024),
            name='conv_stack',
        )(images, w_a, norm_a, w_down, norm_down, w_b, norm_b)
        n_step = 6
        result = pl.pallas_call(
            norm_kernel,
            out_shape=jax.ShapeDtypeStruct(z_val.shape, BF16),
            in_specs=[any_spec] * 4,
            out_specs=any_spec,
            scratch_shapes=[
                pltpu.VMEM(z_val.shape, F32),
                pltpu.VMEM((3, 1, ch_b), F32),
                pltpu.VMEM(z_val.shape, BF16),
                pltpu.SemaphoreType.DMA((n_step,)),
                pltpu.SemaphoreType.DMA((3,)),
                pltpu.SemaphoreType.DMA((n_step,)),
            ],
            compiler_params=pltpu.CompilerParams(vmem_limit_bytes=60 * 1024 * 1024),
            name='last_norm',
        )(z_val, mean, gain, beta)
        return jnp.transpose(result, (0, 2, 1, 3))

    act_spec = P(('pod', 'dp'), 'sp', None, None)
    return jax.shard_map(local_stack, mesh=mesh, in_specs=(act_spec, P(), P(), P(), P(), P(), P()), out_specs=act_spec, check_vma=False)
```

```python
import functools

import jax
import jax.numpy as jnp
from jax import lax
from jax.experimental import pallas as pl
from jax.experimental.pallas import tpu as pltpu
from jax.sharding import PartitionSpec as P

EPS_VALUE = 1e-5
MESH_ID = pl.DeviceIdType.MESH
LANES = 128
GUARD = 8
F32 = jnp.float32
BF16 = jnp.bfloat16


def stack_kernel(data_size, group_size, images, w_a, norm_a, w_down, norm_down, w_b, norm_b, z_out, mean_out, gain_out, beta_out,
                 x_in, w_a_in, w_down_in, w_b_in, norm_a_in, norm_down_in, norm_b_in, wide_a, wide_down, wide_b,
                 send_low, send_up, from_up, from_low, pixels, masks, taps, z_a, z_mid, z_down, z_b, z_last, z_turned, scale_rows,
                 parts, slots, in_sems, w_sems, out_sems, image_send, image_recv, z_send, z_recv, sum_send, sum_recv):
    n_img, rows, width, _ = images.shape
    half = width // 2
    last_stride = n_img * half + 1
    block = n_img * half
    pairs = rows // 2
    total = data_size * group_size
    dp_idx = lax.axis_index('dp')
    sp_idx = lax.axis_index('sp')
    me = dp_idx * group_size + sp_idx
    is_top = sp_idx == 0
    is_bottom = sp_idx == group_size - 1
    keep_top = jnp.where(is_top, 0.0, 1.0).astype(F32)
    keep_bottom = jnp.where(is_bottom, 0.0, 1.0).astype(F32)

    ring = group_size // 2

    def distance(peer):
        return min(peer[0], data_size - peer[0]) + min(peer[1], ring - peer[1])

    offsets = [(d, x, c) for d in range(data_size) for x in range(ring) for c in range(2)][1:]
    offsets.sort(key=distance, reverse=True)

    def peer_of(offset):
        core = lax.rem(sp_idx, 2)
        place = lax.rem(sp_idx // 2 + offset[1], ring)
        return {'dp': lax.rem(dp_idx + offset[0], data_size), 'sp': place * 2 + (1 - core if offset[2] else core)}

    n_chunk = in_sems.shape[0]
    chunk = rows // n_chunk

    def image_copy(idx):
        return pltpu.make_async_copy(images.at[:, pl.ds(idx * chunk, chunk)], x_in.at[:, pl.ds(idx * chunk, chunk)], in_sems.at[idx])

    image_copy(0).start()
    image_copy(n_chunk - 1).start()
    barrier = pltpu.get_barrier_semaphore()
    for offset in offsets:
        pl.semaphore_signal(barrier, inc=1, device_id=peer_of(offset), device_id_type=MESH_ID)
    for idx in range(1, n_chunk - 1):
        image_copy(idx).start()
    small_pairs = [(w_a, w_a_in), (norm_a, norm_a_in), (w_down, w_down_in), (norm_down, norm_down_in), (w_b, w_b_in), (norm_b, norm_b_in)]
    small_copies = [pltpu.make_async_copy(src, dst, w_sems.at[idx]) for idx, (src, dst) in enumerate(small_pairs)]
    for copy in small_copies:
        copy.start()

    pos = lax.rem(lax.broadcasted_iota(jnp.int32, (block, LANES), 0), half)
    masks[0] = (pos != 0).astype(F32)
    masks[1] = (pos != half - 1).astype(F32)
    pixels[0:GUARD] = jnp.zeros((GUARD, LANES), F32)
    pixels[GUARD + n_img * width:] = jnp.zeros((GUARD, LANES), F32)

    def clear_guards(ref, outer):
        def body(idx, carry):
            view = ref.at[idx]
            view[0:GUARD] = jnp.zeros((GUARD, LANES), F32)
            view[GUARD + block:] = jnp.zeros((GUARD, LANES), F32)
            return carry
        lax.fori_loop(0, outer, body, 0)


    def clear_inner(ref):
        def body(idx, carry):
            view = ref.at[idx]
            view[0:GUARD] = jnp.zeros((GUARD, LANES), F32)
            view[GUARD + block:] = jnp.zeros((GUARD, LANES), F32)
            return carry
        lax.fori_loop(1, pairs + 1, body, 0)

    @pl.when(is_top)
    def _():
        from_up[...] = jnp.zeros(from_up.shape, BF16)

    @pl.when(is_bottom)
    def _():
        from_low[...] = jnp.zeros(from_low.shape, BF16)

    waited = set()

    def need_row(row):
        idx = row // chunk
        if idx not in waited:
            waited.add(idx)
            image_copy(idx).wait()

    for row in (0, rows - 1):
        need_row(row)
    plane = n_img * width

    def packed_row(row):
        halves = [x_in[pl.ds(idx * (n_img // 2), n_img // 2), row].astype(F32) for idx in range(2)]
        return jnp.concatenate(halves, axis=2).reshape(plane // 2, LANES).astype(BF16)

    for idx in range(2):
        send_low[idx] = packed_row(rows - 1 - idx)
    for idx in range(3):
        send_up[idx] = packed_row(idx)

    def image_copies(down, part):
        src, dst = (send_low, from_up) if down else (send_up, from_low)
        span = pl.ds(0, 1) if part == 0 else pl.ds(1, src.shape[0] - 1)
        place = 2 * part + (0 if down else 1)
        return pltpu.make_async_remote_copy(src_ref=src.at[span], dst_ref=dst.at[span], send_sem=image_send.at[place], recv_sem=image_recv.at[place],
                                            device_id={'sp': sp_idx + 1 if down else sp_idx - 1}, device_id_type=MESH_ID)

    def send_images():
        @pl.when(jnp.logical_not(is_bottom))
        def _():
            image_copies(True, 0).start()
            image_copies(True, 1).start()

        @pl.when(jnp.logical_not(is_top))
        def _():
            image_copies(False, 0).start()
            image_copies(False, 1).start()

    def recv_images(part):
        @pl.when(jnp.logical_not(is_top))
        def _():
            image_copies(True, part).wait_recv()

        @pl.when(jnp.logical_not(is_bottom))
        def _():
            image_copies(False, part).wait_recv()

    def finish_images():
        @pl.when(jnp.logical_not(is_bottom))
        def _():
            image_copies(True, 0).wait_send()
            image_copies(True, 1).wait_send()

        @pl.when(jnp.logical_not(is_top))
        def _():
            image_copies(False, 0).wait_send()
            image_copies(False, 1).wait_send()

    ch_a = w_a.shape[3]
    zero_a = jnp.zeros((ch_a, ch_a), BF16)
    zero_b = jnp.zeros((LANES, LANES), BF16)
    zero_d = jnp.zeros((ch_a, LANES), BF16)

    def tap_a(layer, p, q):
        return w_a_in[layer, p, q] if 0 <= p <= 2 and 0 <= q <= 2 else zero_a

    def widen_a(layer):
        for q in range(4):
            for t in range(4):
                for dw in range(2):
                    both = jnp.concatenate([tap_a(layer, t, q - dw), tap_a(layer, t - 1, q - dw)], axis=1)
                    wide_a[layer, pl.ds((q * 4 + t) * ch_a, ch_a), pl.ds(dw * LANES, LANES)] = both

    def widen_down():
        for q in range(3):
            for t in range(6):
                for d in range(2):
                    p = t - 1 - 2 * d
                    wide_down[pl.ds((q * 6 + t) * ch_a, ch_a), pl.ds(d * LANES, LANES)] = w_down_in[p, q] if 0 <= p <= 2 else zero_d

    def widen_b():
        for layer in range(2):
            for q in range(3):
                for t in range(4):
                    for d in range(2):
                        p = t - d
                        wide_b[layer, pl.ds((q * 4 + t) * LANES, LANES), pl.ds(d * LANES, LANES)] = w_b_in[layer, p, q] if 0 <= p <= 2 else zero_b

    def image_row(row):
        half_a = LANES // 2
        if row < -2:
            return jnp.zeros((plane, half_a), F32)
        if 0 <= row < rows:
            need_row(row)
            return x_in[:, row].astype(F32).reshape(plane, half_a)
        packed = (from_up[-1 - row] if row < 0 else from_low[row - rows]).astype(F32)
        return jnp.concatenate([packed[:, :half_a], packed[:, half_a:]], axis=0)

    def spread_pair(p):
        both = jnp.concatenate([image_row(2 * p - 3), image_row(2 * p - 2)], axis=1)
        pixels[pl.ds(GUARD, n_img * width)] = both
        taps[0, p] = (pixels[pl.ds(GUARD - 1, block, stride=2)] * masks[0]).astype(BF16)
        taps[1, p] = pixels[pl.ds(GUARD, block, stride=2)].astype(BF16)
        taps[2, p] = pixels[pl.ds(GUARD + 1, block, stride=2)].astype(BF16)
        taps[3, p] = (pixels[pl.ds(GUARD + 2, block, stride=2)] * masks[1]).astype(BF16)

    def conv_a(layer, idx, dst):
        left = jnp.concatenate([taps[q, idx + s] for q in range(4) for s in range(2)], axis=1)
        z_val = jnp.dot(left, wide_a[layer], preferred_element_type=F32)
        dst[idx, pl.ds(GUARD, block)] = z_val[:, :LANES]
        dst[idx + dst.shape[0] // 2, pl.ds(GUARD, block)] = z_val[:, LANES:]
        return z_val

    def conv_down(idx):
        left = jnp.concatenate([taps[q, 2 * idx + s] for q in range(1, 4) for s in range(3)], axis=1)
        z_val = jnp.dot(left, wide_down[...], preferred_element_type=F32)
        z_down[2 * idx + 1, pl.ds(GUARD, block)] = z_val[:, :LANES]
        z_down[2 * idx + 2, pl.ds(GUARD, block)] = z_val[:, LANES:]
        return z_val

    def conv_b(layer, idx):
        left = jnp.concatenate([taps[q, 2 * idx + t] for q in range(3) for t in range(4)], axis=1)
        z_val = jnp.dot(left, wide_b[layer], preferred_element_type=F32)
        if layer == 0:
            z_b[2 * idx + 1, pl.ds(GUARD, block)] = z_val[:, :LANES]
            z_b[2 * idx + 2, pl.ds(GUARD, block)] = z_val[:, LANES:]
        else:
            z_last[pl.ds(2 * idx * last_stride, block)] = z_val[:, :LANES]
            z_last[pl.ds((2 * idx + 1) * last_stride, block)] = z_val[:, LANES:]
        return z_val

    def run(tap_order, conv_order, need, make_taps, conv, sums):
        made = 0
        for idx, count in zip(conv_order, need):
            for tap in tap_order[made:count]:
                make_taps(tap)
            made = max(made, count)
            sums = conv(idx, sums)
        return sums

    def add_sums(sums, z_val):
        tiles = z_val.reshape(block // 8, 8, 2 * LANES)
        return sums[0] + jnp.sum(tiles, axis=0), sums[1] + jnp.sum(tiles * tiles, axis=0)

    zero_sums = (jnp.zeros((8, 2 * LANES), F32), jnp.zeros((8, 2 * LANES), F32))

    def fold_sums(sums):
        rows_sum = [jnp.sum(val, axis=0, keepdims=True) for val in sums]
        return jnp.concatenate([val[:, :LANES] + val[:, LANES:] for val in rows_sum], axis=0)

    def sum_copy(layer, offset):
        return pltpu.make_async_remote_copy(src_ref=parts.at[layer], dst_ref=slots.at[layer, me], send_sem=sum_send.at[layer],
                                            recv_sem=sum_recv.at[layer], device_id=peer_of(offset), device_id_type=MESH_ID)

    def send_sums(layer, part):
        parts[layer] = part
        slots[layer, me] = part
        for offset in offsets:
            sum_copy(layer, offset).start()

    def group_sum(layer):
        others = slots.at[layer, pl.ds(0, total - 1)]
        pltpu.make_async_copy(others, others, sum_recv.at[layer]).wait()
        return jnp.sum(slots[layer], axis=0)

    def finish_sum(layer):
        others = slots.at[layer, pl.ds(0, total - 1)]
        pltpu.make_async_copy(others, others, sum_send.at[layer]).wait()

    def scales(sums, count, gamma, beta):
        mean = sums[0:1] / count
        var = sums[1:2] / count - mean * mean
        return mean, gamma * lax.rsqrt(var + EPS_VALUE), beta

    def scales_a(sums, count, pair):
        both = sums + jnp.concatenate([sums[:, LANES // 2:], sums[:, :LANES // 2]], axis=1)
        twice = jnp.concatenate([pair, pair], axis=1)
        return scales(both, count, twice[0:1], twice[1:2])

    def normed(z_val, scale, keep=None):
        mean, gain, beta = scale
        if keep is not None:
            gain, beta = gain * keep, beta * keep
        return jnp.maximum((z_val - mean) * gain + beta, 0.0)

    lane = lax.broadcasted_iota(jnp.int32, (1, LANES), 1)
    upper_half = (lane < LANES // 2).astype(F32)
    lower_half = 1.0 - upper_half

    small_copies[0].wait()
    widen_a(0)

    def conv_first(idx, acc):
        return add_sums(acc, conv_a(0, idx, z_a))

    early = chunk // 2
    sums = run(range(2, early + 1), range(2, early), range(2, early), spread_pair, conv_first, zero_sums)
    pl.semaphore_wait(barrier, total - 1)
    send_images()
    for row in range(0, rows, chunk):
        need_row(row)
    last = pairs - 2
    sums = run(range(early + 1, last + 3), range(early, last + 2), range(1, last - early + 3), spread_pair, conv_first, sums)
    recv_images(0)
    sums = run([1, pairs + 1], [1, pairs], [1, 2], spread_pair, conv_first, sums)
    send_sums(0, fold_sums(sums))
    recv_images(1)
    spread_pair(0)
    conv_a(0, 0, z_a)
    spread_pair(pairs + 2)
    conv_a(0, pairs + 1, z_a)
    for copy in small_copies[1:]:
        copy.wait()
    widen_a(1)
    widen_down()
    widen_b()
    clear_guards(z_a, z_a.shape[0])
    clear_guards(z_mid, z_mid.shape[0])
    clear_inner(z_down)
    clear_inner(z_b)
    count_a = n_img * rows * width * total
    scale = scales_a(group_sum(0), count_a, norm_a_in[0])

    def taps_mid(idx, src, scale, keep, left=True):
        odd = idx + src.shape[0] // 2
        if left:
            taps[0, idx] = (normed(src[odd, pl.ds(GUARD - 1, block)], scale, keep) * masks[0]).astype(BF16)
        taps[1, idx] = normed(src[idx, pl.ds(GUARD, block)], scale, keep).astype(BF16)
        taps[2, idx] = normed(src[odd, pl.ds(GUARD, block)], scale, keep).astype(BF16)
        taps[3, idx] = (normed(src[idx, pl.ds(GUARD + 1, block)], scale, keep) * masks[1]).astype(BF16)

    def keep_pairs(idx):
        return keep_top if idx == 0 else keep_bottom if idx == pairs + 1 else None

    def conv_second(idx, acc):
        z_val = conv_a(1, idx, z_mid)
        if idx in (0, pairs):
            own = lower_half if idx == 0 else upper_half
            own = jnp.concatenate([own, own], axis=1)
            new = add_sums(zero_sums, z_val)
            return acc[0] + own * new[0], acc[1] + own * new[1]
        return add_sums(acc, z_val)

    sums = run(range(pairs + 2), range(pairs + 1), range(2, pairs + 3), lambda idx: taps_mid(idx, z_a, scale, keep_pairs(idx)), conv_second, zero_sums)
    send_sums(1, fold_sums(sums))
    scale_mid = scales_a(group_sum(1), count_a, norm_a_in[1])

    def keep_staggered(idx):
        return upper_half + lower_half * keep_bottom if idx == pairs else None

    def edge_copies(ref, slot):
        below = pltpu.make_async_remote_copy(src_ref=ref.at[pairs], dst_ref=ref.at[0], send_sem=z_send.at[slot, 0], recv_sem=z_recv.at[slot, 0],
                                             device_id={'sp': lax.rem(sp_idx + 1, group_size)}, device_id_type=MESH_ID)
        above = pltpu.make_async_remote_copy(src_ref=ref.at[1], dst_ref=ref.at[pairs + 1], send_sem=z_send.at[slot, 1], recv_sem=z_recv.at[slot, 1],
                                             device_id={'sp': lax.rem(sp_idx + group_size - 1, group_size)}, device_id_type=MESH_ID)
        return below, above

    def send_edges(ref, slot):
        for copy in edge_copies(ref, slot):
            copy.start()

    def recv_edges(ref, slot):
        for copy in edge_copies(ref, slot):
            copy.wait_recv()

    def finish_edges(ref, slot):
        for copy in edge_copies(ref, slot):
            copy.wait_send()

    count_b = n_img * pairs * half * total
    last = pairs // 2 - 1
    def conv_third(idx, acc):
        return add_sums(acc, conv_down(idx))

    sums = run(range(pairs + 1), range(last + 1), range(3, pairs + 2, 2), lambda idx: taps_mid(idx, z_mid, scale_mid, keep_staggered(idx), left=False), conv_third, zero_sums)
    send_sums(2, fold_sums(sums))
    send_edges(z_down, 0)
    scale_down = scales(group_sum(2), count_b, norm_down_in[0:1], norm_down_in[1:2])
    recv_edges(z_down, 0)

    def taps_low(idx, src, scale):
        keep = keep_pairs(idx)
        taps[0, idx] = (normed(src[idx, pl.ds(GUARD - 1, block)], scale, keep) * masks[0]).astype(BF16)
        taps[1, idx] = normed(src[idx, pl.ds(GUARD, block)], scale, keep).astype(BF16)
        taps[2, idx] = (normed(src[idx, pl.ds(GUARD + 1, block)], scale, keep) * masks[1]).astype(BF16)

    def conv_fourth(idx, acc):
        return add_sums(acc, conv_b(0, idx))

    def conv_fifth(idx, acc):
        return add_sums(acc, conv_b(1, idx))

    sums = run(range(pairs + 2), range(last + 1), range(4, pairs + 3, 2), lambda idx: taps_low(idx, z_down, scale_down), conv_fourth, zero_sums)
    send_sums(3, fold_sums(sums))
    send_edges(z_b, 1)
    scale_b = scales(group_sum(3), count_b, norm_b_in[0, 0:1], norm_b_in[0, 1:2])
    recv_edges(z_b, 1)
    sums = run(range(pairs + 2), range(last + 1), range(4, pairs + 3, 2), lambda idx: taps_low(idx, z_b, scale_b), conv_fifth, zero_sums)
    send_sums(4, fold_sums(sums))

    n_out = out_sems.shape[0] - 3
    out_chunk = n_img // n_out

    def out_copy(idx):
        part = pl.ds(idx * out_chunk, out_chunk)
        return pltpu.make_async_copy(z_turned.at[part], z_out.at[part], out_sems.at[idx])

    def turn(img, carry):
        for col in range(half):
            z_turned[img, col] = z_last[pl.ds(img * half + col, pairs, stride=last_stride)]
        return carry

    for idx in range(n_out):
        lax.fori_loop(idx * out_chunk, (idx + 1) * out_chunk, turn, 0)
        out_copy(idx).start()
    mean, gain, beta = scales(group_sum(4), count_b, norm_b_in[1, 0:1], norm_b_in[1, 1:2])
    scale_copies = []
    for idx, (val, dst) in enumerate([(mean, mean_out), (gain, gain_out), (beta, beta_out)]):
        scale_rows[idx] = val
        scale_copies.append(pltpu.make_async_copy(scale_rows.at[idx], dst, out_sems.at[n_out + idx]))
    for copy in scale_copies:
        copy.start()

    finish_images()
    finish_edges(z_down, 0)
    finish_edges(z_b, 1)
    for layer in range(5):
        finish_sum(layer)
    for idx in range(n_out):
        out_copy(idx).wait()
    for copy in scale_copies:
        copy.wait()


def norm_kernel(z_hbm, mean_hbm, gain_hbm, beta_hbm, out_hbm, z_ref, rows_ref, out_ref, z_sems, row_sems, out_sems):
    n_step = z_sems.shape[0]
    size = z_ref.shape[0] // n_step
    row_copies = [pltpu.make_async_copy(src, rows_ref.at[idx], row_sems.at[idx]) for idx, src in enumerate((mean_hbm, gain_hbm, beta_hbm))]
    parts = [pl.ds(idx * size, size) for idx in range(n_step)]
    z_copies = [pltpu.make_async_copy(z_hbm.at[part], z_ref.at[part], z_sems.at[idx]) for idx, part in enumerate(parts)]
    out_copies = [pltpu.make_async_copy(out_ref.at[part], out_hbm.at[part], out_sems.at[idx]) for idx, part in enumerate(parts)]
    for copy in row_copies + z_copies:
        copy.start()
    for copy in row_copies:
        copy.wait()
    for part, z_copy, out_copy in zip(parts, z_copies, out_copies):
        z_copy.wait()
        out_ref[part] = jnp.maximum((z_ref[part] - rows_ref[0]) * rows_ref[1] + rows_ref[2], 0.0).astype(BF16)
        out_copy.start()
    for copy in out_copies:
        copy.wait()


def solution(mesh):
    group_size = mesh.shape['sp']
    data_size = mesh.shape['dp']
    total = data_size * group_size

    def local_stack(images, w_a, norm_a, w_down, norm_down, w_b, norm_b):
        n_img, rows, width, ch_a = images.shape
        ch_b = w_down.shape[3]
        pairs, half = rows // 2, width // 2
        block = n_img * half
        padded = block + 2 * GUARD
        any_spec = pl.BlockSpec(memory_space=pl.ANY)
        n_chunk, n_out = 4, 4
        z_val, mean, gain, beta = pl.pallas_call(
            functools.partial(stack_kernel, data_size, group_size),
            out_shape=(jax.ShapeDtypeStruct((n_img, half, pairs, ch_b), F32),) + (jax.ShapeDtypeStruct((1, LANES), F32),) * 3,
            in_specs=[any_spec] * 7,
            out_specs=(any_spec,) * 4,
            scratch_shapes=[
                pltpu.VMEM((n_img, rows, width, ch_a), BF16),
                pltpu.VMEM(w_a.shape, BF16),
                pltpu.VMEM(w_down.shape, BF16),
                pltpu.VMEM(w_b.shape, BF16),
                pltpu.VMEM(norm_a.shape, F32),
                pltpu.VMEM(norm_down.shape, F32),
                pltpu.VMEM(norm_b.shape, F32),
                pltpu.VMEM((2, 16 * ch_a, 2 * LANES), BF16),
                pltpu.VMEM((18 * ch_a, 2 * LANES), BF16),
                pltpu.VMEM((2, 12 * ch_b, 2 * LANES), BF16),
                pltpu.VMEM((2, n_img * width // 2, LANES), BF16),
                pltpu.VMEM((3, n_img * width // 2, LANES), BF16),
                pltpu.VMEM((2, n_img * width // 2, LANES), BF16),
                pltpu.VMEM((3, n_img * width // 2, LANES), BF16),
                pltpu.VMEM((n_img * width + 2 * GUARD, LANES), F32),
                pltpu.VMEM((2, block, LANES), F32),
                pltpu.VMEM((4, pairs + 3, block, LANES), BF16),
                pltpu.VMEM((2 * (pairs + 2), padded, LANES), F32),
                pltpu.VMEM((2 * (pairs + 1), padded, LANES), F32),
                pltpu.VMEM((pairs + 2, padded, LANES), F32),
                pltpu.VMEM((pairs + 2, padded, LANES), F32),
                pltpu.VMEM((pairs * (block + 1) + 7, LANES), F32),
                pltpu.VMEM((n_img, half, pairs, ch_b), F32),
                pltpu.VMEM((3, 1, LANES), F32),
                pltpu.VMEM((5, 2, LANES), F32),
                pltpu.VMEM((5, total, 2, LANES), F32),
                pltpu.SemaphoreType.DMA((n_chunk,)),
                pltpu.SemaphoreType.DMA((6,)),
                pltpu.SemaphoreType.DMA((n_out + 3,)),
                pltpu.SemaphoreType.DMA((4,)),
                pltpu.SemaphoreType.DMA((4,)),
                pltpu.SemaphoreType.DMA((2, 2)),
                pltpu.SemaphoreType.DMA((2, 2)),
                pltpu.SemaphoreType.DMA((5,)),
                pltpu.SemaphoreType.DMA((5,)),
            ],
            compiler_params=pltpu.CompilerParams(collective_id=0, has_side_effects=True, vmem_limit_bytes=60 * 1024 * 1024),
            name='conv_stack',
        )(images, w_a, norm_a, w_down, norm_down, w_b, norm_b)
        n_step = 6
        result = pl.pallas_call(
            norm_kernel,
            out_shape=jax.ShapeDtypeStruct(z_val.shape, BF16),
            in_specs=[any_spec] * 4,
            out_specs=any_spec,
            scratch_shapes=[
                pltpu.VMEM(z_val.shape, F32),
                pltpu.VMEM((3, 1, ch_b), F32),
                pltpu.VMEM(z_val.shape, BF16),
                pltpu.SemaphoreType.DMA((n_step,)),
                pltpu.SemaphoreType.DMA((3,)),
                pltpu.SemaphoreType.DMA((n_step,)),
            ],
            compiler_params=pltpu.CompilerParams(vmem_limit_bytes=60 * 1024 * 1024),
            name='last_norm',
        )(z_val, mean, gain, beta)
        return jnp.transpose(result, (0, 2, 1, 3))

    act_spec = P(('pod', 'dp'), 'sp', None, None)
    return jax.shard_map(local_stack, mesh=mesh, in_specs=(act_spec, P(), P(), P(), P(), P(), P()), out_specs=act_spec, check_vma=False)
```

```python
import functools

import jax
import jax.numpy as jnp
from jax import lax
from jax.experimental import pallas as pl
from jax.experimental.pallas import tpu as pltpu
from jax.sharding import PartitionSpec as P

EPS_VALUE = 1e-5
MESH_ID = pl.DeviceIdType.MESH
LANES = 128
GUARD = 8
F32 = jnp.float32
BF16 = jnp.bfloat16


def stack_kernel(data_size, group_size, images, w_a, norm_a, w_down, norm_down, w_b, norm_b, z_out, mean_out, gain_out, beta_out,
                 x_in, w_a_in, w_down_in, w_b_in, norm_a_in, norm_down_in, norm_b_in, wide_a, wide_down, wide_b,
                 send_low, send_up, from_up, from_low, pixels, masks, taps, z_a, z_mid, z_down, z_b, z_last, z_turned, scale_rows,
                 parts, slots, in_sems, w_sems, out_sems, image_send, image_recv, z_send, z_recv, sum_send, sum_recv):
    n_img, rows, width, _ = images.shape
    half = width // 2
    last_stride = n_img * half + 1
    block = n_img * half
    pairs = rows // 2
    total = data_size * group_size
    dp_idx = lax.axis_index('dp')
    sp_idx = lax.axis_index('sp')
    me = dp_idx * group_size + sp_idx
    is_top = sp_idx == 0
    is_bottom = sp_idx == group_size - 1
    keep_top = jnp.where(is_top, 0.0, 1.0).astype(F32)
    keep_bottom = jnp.where(is_bottom, 0.0, 1.0).astype(F32)

    ring = group_size // 2

    def distance(peer):
        return min(peer[0], data_size - peer[0]) + min(peer[1], ring - peer[1])

    offsets = [(d, x, c) for d in range(data_size) for x in range(ring) for c in range(2)][1:]
    offsets.sort(key=distance, reverse=True)

    def peer_of(offset):
        core = lax.rem(sp_idx, 2)
        place = lax.rem(sp_idx // 2 + offset[1], ring)
        return {'dp': lax.rem(dp_idx + offset[0], data_size), 'sp': place * 2 + (1 - core if offset[2] else core)}

    n_chunk = in_sems.shape[0]
    chunk = rows // n_chunk

    def image_copy(idx):
        return pltpu.make_async_copy(images.at[:, pl.ds(idx * chunk, chunk)], x_in.at[:, pl.ds(idx * chunk, chunk)], in_sems.at[idx])

    image_copy(0).start()
    image_copy(n_chunk - 1).start()
    barrier = pltpu.get_barrier_semaphore()
    for offset in offsets:
        pl.semaphore_signal(barrier, inc=1, device_id=peer_of(offset), device_id_type=MESH_ID)
    for idx in range(1, n_chunk - 1):
        image_copy(idx).start()
    small_pairs = [(w_a, w_a_in), (norm_a, norm_a_in), (w_down, w_down_in), (norm_down, norm_down_in), (w_b, w_b_in), (norm_b, norm_b_in)]
    small_copies = [pltpu.make_async_copy(src, dst, w_sems.at[idx]) for idx, (src, dst) in enumerate(small_pairs)]
    for copy in small_copies:
        copy.start()

    pos = lax.rem(lax.broadcasted_iota(jnp.int32, (block, LANES), 0), half)
    masks[0] = (pos != 0).astype(F32)
    masks[1] = (pos != half - 1).astype(F32)
    pixels[0:GUARD] = jnp.zeros((GUARD, LANES), F32)
    pixels[GUARD + n_img * width:] = jnp.zeros((GUARD, LANES), F32)

    def clear_guards(ref, outer):
        def body(idx, carry):
            view = ref.at[idx]
            view[0:GUARD] = jnp.zeros((GUARD, LANES), F32)
            view[GUARD + block:] = jnp.zeros((GUARD, LANES), F32)
            return carry
        lax.fori_loop(0, outer, body, 0)


    def clear_inner(ref):
        def body(idx, carry):
            view = ref.at[idx]
            view[0:GUARD] = jnp.zeros((GUARD, LANES), F32)
            view[GUARD + block:] = jnp.zeros((GUARD, LANES), F32)
            return carry
        lax.fori_loop(1, pairs + 1, body, 0)

    @pl.when(is_top)
    def _():
        from_up[...] = jnp.zeros(from_up.shape, BF16)

    @pl.when(is_bottom)
    def _():
        from_low[...] = jnp.zeros(from_low.shape, BF16)

    waited = set()

    def need_row(row):
        idx = row // chunk
        if idx not in waited:
            waited.add(idx)
            image_copy(idx).wait()

    for row in (0, rows - 1):
        need_row(row)
    plane = n_img * width

    def packed_row(row):
        halves = [x_in[pl.ds(idx * (n_img // 2), n_img // 2), row].astype(F32) for idx in range(2)]
        return jnp.concatenate(halves, axis=2).reshape(plane // 2, LANES).astype(BF16)

    for idx in range(2):
        send_low[idx] = packed_row(rows - 1 - idx)
    for idx in range(3):
        send_up[idx] = packed_row(idx)

    def image_copies(down, part):
        src, dst = (send_low, from_up) if down else (send_up, from_low)
        span = pl.ds(0, 1) if part == 0 else pl.ds(1, src.shape[0] - 1)
        place = 2 * part + (0 if down else 1)
        return pltpu.make_async_remote_copy(src_ref=src.at[span], dst_ref=dst.at[span], send_sem=image_send.at[place], recv_sem=image_recv.at[place],
                                            device_id={'sp': sp_idx + 1 if down else sp_idx - 1}, device_id_type=MESH_ID)

    def send_images():
        @pl.when(jnp.logical_not(is_bottom))
        def _():
            image_copies(True, 0).start()
            image_copies(True, 1).start()

        @pl.when(jnp.logical_not(is_top))
        def _():
            image_copies(False, 0).start()
            image_copies(False, 1).start()

    def recv_images(part):
        @pl.when(jnp.logical_not(is_top))
        def _():
            image_copies(True, part).wait_recv()

        @pl.when(jnp.logical_not(is_bottom))
        def _():
            image_copies(False, part).wait_recv()

    def finish_images():
        @pl.when(jnp.logical_not(is_bottom))
        def _():
            image_copies(True, 0).wait_send()
            image_copies(True, 1).wait_send()

        @pl.when(jnp.logical_not(is_top))
        def _():
            image_copies(False, 0).wait_send()
            image_copies(False, 1).wait_send()

    ch_a = w_a.shape[3]
    zero_a = jnp.zeros((ch_a, ch_a), BF16)
    zero_b = jnp.zeros((LANES, LANES), BF16)
    zero_d = jnp.zeros((ch_a, LANES), BF16)

    def tap_a(layer, p, q):
        return w_a_in[layer, p, q] if 0 <= p <= 2 and 0 <= q <= 2 else zero_a

    def widen_a(layer):
        for q in range(4):
            for t in range(4):
                for dw in range(2):
                    both = jnp.concatenate([tap_a(layer, t, q - dw), tap_a(layer, t - 1, q - dw)], axis=1)
                    wide_a[layer, pl.ds((q * 4 + t) * ch_a, ch_a), pl.ds(dw * LANES, LANES)] = both

    def widen_down():
        for q in range(3):
            for t in range(6):
                for d in range(2):
                    p = t - 1 - 2 * d
                    wide_down[pl.ds((q * 6 + t) * ch_a, ch_a), pl.ds(d * LANES, LANES)] = w_down_in[p, q] if 0 <= p <= 2 else zero_d

    def widen_b():
        for layer in range(2):
            for q in range(3):
                for t in range(4):
                    for d in range(2):
                        p = t - d
                        wide_b[layer, pl.ds((q * 4 + t) * LANES, LANES), pl.ds(d * LANES, LANES)] = w_b_in[layer, p, q] if 0 <= p <= 2 else zero_b

    def image_row(row):
        half_a = LANES // 2
        if row < -2:
            return jnp.zeros((plane, half_a), F32)
        if 0 <= row < rows:
            need_row(row)
            return x_in[:, row].astype(F32).reshape(plane, half_a)
        packed = (from_up[-1 - row] if row < 0 else from_low[row - rows]).astype(F32)
        return jnp.concatenate([packed[:, :half_a], packed[:, half_a:]], axis=0)

    def spread_pair(p):
        both = jnp.concatenate([image_row(2 * p - 3), image_row(2 * p - 2)], axis=1)
        pixels[pl.ds(GUARD, n_img * width)] = both
        taps[0, p] = (pixels[pl.ds(GUARD - 1, block, stride=2)] * masks[0]).astype(BF16)
        taps[1, p] = pixels[pl.ds(GUARD, block, stride=2)].astype(BF16)
        taps[2, p] = pixels[pl.ds(GUARD + 1, block, stride=2)].astype(BF16)
        taps[3, p] = (pixels[pl.ds(GUARD + 2, block, stride=2)] * masks[1]).astype(BF16)

    def conv_a(layer, idx, dst):
        left = jnp.concatenate([taps[q, idx + s] for q in range(4) for s in range(2)], axis=1)
        z_val = jnp.dot(left, wide_a[layer], preferred_element_type=F32)
        dst[idx, pl.ds(GUARD, block)] = z_val[:, :LANES]
        dst[idx + dst.shape[0] // 2, pl.ds(GUARD, block)] = z_val[:, LANES:]
        return z_val

    def conv_down(idx):
        left = jnp.concatenate([taps[q, 2 * idx + s] for q in range(1, 4) for s in range(3)], axis=1)
        z_val = jnp.dot(left, wide_down[...], preferred_element_type=F32)
        z_down[2 * idx + 1, pl.ds(GUARD, block)] = z_val[:, :LANES]
        z_down[2 * idx + 2, pl.ds(GUARD, block)] = z_val[:, LANES:]
        return z_val

    def conv_b(layer, idx):
        left = jnp.concatenate([taps[q, 2 * idx + t] for q in range(3) for t in range(4)], axis=1)
        z_val = jnp.dot(left, wide_b[layer], preferred_element_type=F32)
        if layer == 0:
            z_b[2 * idx + 1, pl.ds(GUARD, block)] = z_val[:, :LANES]
            z_b[2 * idx + 2, pl.ds(GUARD, block)] = z_val[:, LANES:]
        else:
            z_last[pl.ds(2 * idx * last_stride, block)] = z_val[:, :LANES]
            z_last[pl.ds((2 * idx + 1) * last_stride, block)] = z_val[:, LANES:]
        return z_val

    def run(tap_order, conv_order, need, make_taps, conv, sums):
        made = 0
        for idx, count in zip(conv_order, need):
            for tap in tap_order[made:count]:
                make_taps(tap)
            made = max(made, count)
            sums = conv(idx, sums)
        return sums

    def add_sums(sums, z_val):
        tiles = z_val.reshape(block // 8, 8, 2 * LANES)
        return sums[0] + jnp.sum(tiles, axis=0), sums[1] + jnp.sum(tiles * tiles, axis=0)

    zero_sums = (jnp.zeros((8, 2 * LANES), F32), jnp.zeros((8, 2 * LANES), F32))

    def fold_sums(sums):
        rows_sum = [jnp.sum(val, axis=0, keepdims=True) for val in sums]
        return jnp.concatenate([val[:, :LANES] + val[:, LANES:] for val in rows_sum], axis=0)

    def sum_copy(layer, offset):
        return pltpu.make_async_remote_copy(src_ref=parts.at[layer], dst_ref=slots.at[layer, me], send_sem=sum_send.at[layer],
                                            recv_sem=sum_recv.at[layer], device_id=peer_of(offset), device_id_type=MESH_ID)

    def send_sums(layer, part):
        parts[layer] = part
        slots[layer, me] = part
        for offset in offsets:
            sum_copy(layer, offset).start()

    def group_sum(layer):
        others = slots.at[layer, pl.ds(0, total - 1)]
        pltpu.make_async_copy(others, others, sum_recv.at[layer]).wait()
        return jnp.sum(slots[layer], axis=0)

    def finish_sum(layer):
        others = slots.at[layer, pl.ds(0, total - 1)]
        pltpu.make_async_copy(others, others, sum_send.at[layer]).wait()

    def scales(sums, count, gamma, beta):
        mean = sums[0:1] / count
        var = sums[1:2] / count - mean * mean
        return mean, gamma * lax.rsqrt(var + EPS_VALUE), beta

    def scales_a(sums, count, pair):
        both = sums + jnp.concatenate([sums[:, LANES // 2:], sums[:, :LANES // 2]], axis=1)
        twice = jnp.concatenate([pair, pair], axis=1)
        return scales(both, count, twice[0:1], twice[1:2])

    def normed(z_val, scale, keep=None):
        mean, gain, beta = scale
        if keep is not None:
            gain, beta = gain * keep, beta * keep
        return jnp.maximum((z_val - mean) * gain + beta, 0.0)

    lane = lax.broadcasted_iota(jnp.int32, (1, LANES), 1)
    upper_half = (lane < LANES // 2).astype(F32)
    lower_half = 1.0 - upper_half

    small_copies[0].wait()
    widen_a(0)

    def conv_first(idx, acc):
        return add_sums(acc, conv_a(0, idx, z_a))

    early = chunk // 2
    sums = run(range(2, early + 1), range(2, early), range(2, early), spread_pair, conv_first, zero_sums)
    pl.semaphore_wait(barrier, total - 1)
    send_images()
    for row in range(0, rows, chunk):
        need_row(row)
    last = pairs - 2
    sums = run(range(early + 1, last + 3), range(early, last + 2), range(1, last - early + 3), spread_pair, conv_first, sums)
    recv_images(0)
    sums = run([1, pairs + 1], [1, pairs], [1, 2], spread_pair, conv_first, sums)
    send_sums(0, fold_sums(sums))
    recv_images(1)
    spread_pair(0)
    conv_a(0, 0, z_a)
    spread_pair(pairs + 2)
    conv_a(0, pairs + 1, z_a)
    for copy in small_copies[1:]:
        copy.wait()
    widen_a(1)
    widen_down()
    widen_b()
    clear_guards(z_a, z_a.shape[0])
    clear_guards(z_mid, z_mid.shape[0])
    clear_inner(z_down)
    clear_inner(z_b)
    count_a = n_img * rows * width * total
    scale = scales_a(group_sum(0), count_a, norm_a_in[0])

    def taps_mid(idx, src, scale, keep, left=True):
        odd = idx + src.shape[0] // 2
        if left:
            taps[0, idx] = (normed(src[odd, pl.ds(GUARD - 1, block)], scale, keep) * masks[0]).astype(BF16)
        taps[1, idx] = normed(src[idx, pl.ds(GUARD, block)], scale, keep).astype(BF16)
        taps[2, idx] = normed(src[odd, pl.ds(GUARD, block)], scale, keep).astype(BF16)
        taps[3, idx] = (normed(src[idx, pl.ds(GUARD + 1, block)], scale, keep) * masks[1]).astype(BF16)

    def keep_pairs(idx):
        return keep_top if idx == 0 else keep_bottom if idx == pairs + 1 else None

    def conv_second(idx, acc):
        z_val = conv_a(1, idx, z_mid)
        if idx in (0, pairs):
            own = lower_half if idx == 0 else upper_half
            own = jnp.concatenate([own, own], axis=1)
            new = add_sums(zero_sums, z_val)
            return acc[0] + own * new[0], acc[1] + own * new[1]
        return add_sums(acc, z_val)

    sums = run(range(pairs + 2), range(pairs + 1), range(2, pairs + 3), lambda idx: taps_mid(idx, z_a, scale, keep_pairs(idx)), conv_second, zero_sums)
    send_sums(1, fold_sums(sums))
    scale_mid = scales_a(group_sum(1), count_a, norm_a_in[1])

    def keep_staggered(idx):
        return upper_half + lower_half * keep_bottom if idx == pairs else None

    def edge_copies(ref, slot):
        below = pltpu.make_async_remote_copy(src_ref=ref.at[pairs], dst_ref=ref.at[0], send_sem=z_send.at[slot, 0], recv_sem=z_recv.at[slot, 0],
                                             device_id={'sp': lax.rem(sp_idx + 1, group_size)}, device_id_type=MESH_ID)
        above = pltpu.make_async_remote_copy(src_ref=ref.at[1], dst_ref=ref.at[pairs + 1], send_sem=z_send.at[slot, 1], recv_sem=z_recv.at[slot, 1],
                                             device_id={'sp': lax.rem(sp_idx + group_size - 1, group_size)}, device_id_type=MESH_ID)
        return below, above

    def send_edges(ref, slot):
        for copy in edge_copies(ref, slot):
            copy.start()

    def recv_edges(ref, slot):
        for copy in edge_copies(ref, slot):
            copy.wait_recv()

    def finish_edges(ref, slot):
        for copy in edge_copies(ref, slot):
            copy.wait_send()

    count_b = n_img * pairs * half * total
    last = pairs // 2 - 1
    def conv_third(idx, acc):
        return add_sums(acc, conv_down(idx))

    sums = run(range(pairs + 1), range(last + 1), range(3, pairs + 2, 2), lambda idx: taps_mid(idx, z_mid, scale_mid, keep_staggered(idx), left=False), conv_third, zero_sums)
    send_sums(2, fold_sums(sums))
    send_edges(z_down, 0)
    scale_down = scales(group_sum(2), count_b, norm_down_in[0:1], norm_down_in[1:2])

    def taps_low(idx, src, scale):
        keep = keep_pairs(idx)
        taps[0, idx] = (normed(src[idx, pl.ds(GUARD - 1, block)], scale, keep) * masks[0]).astype(BF16)
        taps[1, idx] = normed(src[idx, pl.ds(GUARD, block)], scale, keep).astype(BF16)
        taps[2, idx] = (normed(src[idx, pl.ds(GUARD + 1, block)], scale, keep) * masks[1]).astype(BF16)

    def conv_fourth(idx, acc):
        return add_sums(acc, conv_b(0, idx))

    def conv_fifth(idx, acc):
        return add_sums(acc, conv_b(1, idx))

    inner_taps = list(range(2, pairs)) + [1, pairs]
    inner_need = list(range(4, pairs - 3, 2)) + [pairs]

    def run_low(src, slot, scale, conv):
        make = lambda idx: taps_low(idx, src, scale)
        acc = run(inner_taps, range(1, last), inner_need, make, conv, zero_sums)
        recv_edges(src, slot)
        return run([0, pairs + 1], [0, last], [1, 2], make, conv, acc)

    sums = run_low(z_down, 0, scale_down, conv_fourth)
    send_sums(3, fold_sums(sums))
    send_edges(z_b, 1)
    scale_b = scales(group_sum(3), count_b, norm_b_in[0, 0:1], norm_b_in[0, 1:2])
    sums = run_low(z_b, 1, scale_b, conv_fifth)
    send_sums(4, fold_sums(sums))

    n_out = out_sems.shape[0] - 3
    out_chunk = n_img // n_out

    def out_copy(idx):
        part = pl.ds(idx * out_chunk, out_chunk)
        return pltpu.make_async_copy(z_turned.at[part], z_out.at[part], out_sems.at[idx])

    def turn(img, carry):
        for col in range(half):
            z_turned[img, col] = z_last[pl.ds(img * half + col, pairs, stride=last_stride)]
        return carry

    for idx in range(n_out):
        lax.fori_loop(idx * out_chunk, (idx + 1) * out_chunk, turn, 0)
        out_copy(idx).start()
    mean, gain, beta = scales(group_sum(4), count_b, norm_b_in[1, 0:1], norm_b_in[1, 1:2])
    scale_copies = []
    for idx, (val, dst) in enumerate([(mean, mean_out), (gain, gain_out), (beta, beta_out)]):
        scale_rows[idx] = val
        scale_copies.append(pltpu.make_async_copy(scale_rows.at[idx], dst, out_sems.at[n_out + idx]))
    for copy in scale_copies:
        copy.start()

    finish_images()
    finish_edges(z_down, 0)
    finish_edges(z_b, 1)
    for layer in range(5):
        finish_sum(layer)
    for idx in range(n_out):
        out_copy(idx).wait()
    for copy in scale_copies:
        copy.wait()


def norm_kernel(z_hbm, mean_hbm, gain_hbm, beta_hbm, out_hbm, z_ref, rows_ref, out_ref, z_sems, row_sems, out_sems):
    n_step = z_sems.shape[0]
    size = z_ref.shape[0] // n_step
    row_copies = [pltpu.make_async_copy(src, rows_ref.at[idx], row_sems.at[idx]) for idx, src in enumerate((mean_hbm, gain_hbm, beta_hbm))]
    parts = [pl.ds(idx * size, size) for idx in range(n_step)]
    z_copies = [pltpu.make_async_copy(z_hbm.at[part], z_ref.at[part], z_sems.at[idx]) for idx, part in enumerate(parts)]
    out_copies = [pltpu.make_async_copy(out_ref.at[part], out_hbm.at[part], out_sems.at[idx]) for idx, part in enumerate(parts)]
    for copy in row_copies + z_copies:
        copy.start()
    for copy in row_copies:
        copy.wait()
    for part, z_copy, out_copy in zip(parts, z_copies, out_copies):
        z_copy.wait()
        out_ref[part] = jnp.maximum((z_ref[part] - rows_ref[0]) * rows_ref[1] + rows_ref[2], 0.0).astype(BF16)
        out_copy.start()
    for copy in out_copies:
        copy.wait()


def solution(mesh):
    group_size = mesh.shape['sp']
    data_size = mesh.shape['dp']
    total = data_size * group_size

    def local_stack(images, w_a, norm_a, w_down, norm_down, w_b, norm_b):
        n_img, rows, width, ch_a = images.shape
        ch_b = w_down.shape[3]
        pairs, half = rows // 2, width // 2
        block = n_img * half
        padded = block + 2 * GUARD
        any_spec = pl.BlockSpec(memory_space=pl.ANY)
        n_chunk, n_out = 4, 4
        z_val, mean, gain, beta = pl.pallas_call(
            functools.partial(stack_kernel, data_size, group_size),
            out_shape=(jax.ShapeDtypeStruct((n_img, half, pairs, ch_b), F32),) + (jax.ShapeDtypeStruct((1, LANES), F32),) * 3,
            in_specs=[any_spec] * 7,
            out_specs=(any_spec,) * 4,
            scratch_shapes=[
                pltpu.VMEM((n_img, rows, width, ch_a), BF16),
                pltpu.VMEM(w_a.shape, BF16),
                pltpu.VMEM(w_down.shape, BF16),
                pltpu.VMEM(w_b.shape, BF16),
                pltpu.VMEM(norm_a.shape, F32),
                pltpu.VMEM(norm_down.shape, F32),
                pltpu.VMEM(norm_b.shape, F32),
                pltpu.VMEM((2, 16 * ch_a, 2 * LANES), BF16),
                pltpu.VMEM((18 * ch_a, 2 * LANES), BF16),
                pltpu.VMEM((2, 12 * ch_b, 2 * LANES), BF16),
                pltpu.VMEM((2, n_img * width // 2, LANES), BF16),
                pltpu.VMEM((3, n_img * width // 2, LANES), BF16),
                pltpu.VMEM((2, n_img * width // 2, LANES), BF16),
                pltpu.VMEM((3, n_img * width // 2, LANES), BF16),
                pltpu.VMEM((n_img * width + 2 * GUARD, LANES), F32),
                pltpu.VMEM((2, block, LANES), F32),
                pltpu.VMEM((4, pairs + 3, block, LANES), BF16),
                pltpu.VMEM((2 * (pairs + 2), padded, LANES), F32),
                pltpu.VMEM((2 * (pairs + 1), padded, LANES), F32),
                pltpu.VMEM((pairs + 2, padded, LANES), F32),
                pltpu.VMEM((pairs + 2, padded, LANES), F32),
                pltpu.VMEM((pairs * (block + 1) + 7, LANES), F32),
                pltpu.VMEM((n_img, half, pairs, ch_b), F32),
                pltpu.VMEM((3, 1, LANES), F32),
                pltpu.VMEM((5, 2, LANES), F32),
                pltpu.VMEM((5, total, 2, LANES), F32),
                pltpu.SemaphoreType.DMA((n_chunk,)),
                pltpu.SemaphoreType.DMA((6,)),
                pltpu.SemaphoreType.DMA((n_out + 3,)),
                pltpu.SemaphoreType.DMA((4,)),
                pltpu.SemaphoreType.DMA((4,)),
                pltpu.SemaphoreType.DMA((2, 2)),
                pltpu.SemaphoreType.DMA((2, 2)),
                pltpu.SemaphoreType.DMA((5,)),
                pltpu.SemaphoreType.DMA((5,)),
            ],
            compiler_params=pltpu.CompilerParams(collective_id=0, has_side_effects=True, vmem_limit_bytes=60 * 1024 * 1024),
            name='conv_stack',
        )(images, w_a, norm_a, w_down, norm_down, w_b, norm_b)
        n_step = 6
        result = pl.pallas_call(
            norm_kernel,
            out_shape=jax.ShapeDtypeStruct(z_val.shape, BF16),
            in_specs=[any_spec] * 4,
            out_specs=any_spec,
            scratch_shapes=[
                pltpu.VMEM(z_val.shape, F32),
                pltpu.VMEM((3, 1, ch_b), F32),
                pltpu.VMEM(z_val.shape, BF16),
                pltpu.SemaphoreType.DMA((n_step,)),
                pltpu.SemaphoreType.DMA((3,)),
                pltpu.SemaphoreType.DMA((n_step,)),
            ],
            compiler_params=pltpu.CompilerParams(vmem_limit_bytes=60 * 1024 * 1024),
            name='last_norm',
        )(z_val, mean, gain, beta)
        return jnp.transpose(result, (0, 2, 1, 3))

    act_spec = P(('pod', 'dp'), 'sp', None, None)
    return jax.shard_map(local_stack, mesh=mesh, in_specs=(act_spec, P(), P(), P(), P(), P(), P()), out_specs=act_spec, check_vma=False)
```
